8 devices in a mesh: dp: 2 (over y, z), tp: 4 (over x, core).
Axes of the slice: x: 2, y: 2, z: 1, core: 2. Of those that a mesh axis runs over, the one named last changes fastest.
Arguments:
- x: bfloat16 [1536, 6144], P(('dp', 'tp')), parts along dimension 0
- w_gate: bfloat16 [6144, 16384], P(None, 'tp')
- w_up: bfloat16 [6144, 16384], P(None, 'tp')
- w_down: bfloat16 [16384, 6144], P('tp')
Outputs:
- output: bfloat16 [1536, 6144], P(('dp', 'tp')), parts along dimension 0
There are 2 independent parts. The reference program is written for one: setup_inputs(seed, part) draws one part's arguments, and reference() takes and returns one part's arrays. A program takes and returns all parts, laid end to end along the dimension named above; an argument that names none is the same for every part.
All inputs are finite; a program needn't handle non-finite values.
Results may differ from the reference program's by a relative error of at most 0.016.
Values are sent between devices in bfloat16 or wider.
A program may use at most 2 GiB of HBM per device.

```python
import jax
import jax.numpy as jnp

ROWS = 768
D = 6144
FF = 16384


def setup_inputs(seed: int = 0, part: int = 0) -> dict:
    kx, kg, ku, kd = jax.random.split(jax.random.key(seed), 4)
    drawn = {
        "x": jax.random.normal(jax.random.fold_in(kx, part), (ROWS, D), jnp.float32),
        "w_gate": jax.random.normal(kg, (D, FF), jnp.float32) * D**-0.5,
        "w_up": jax.random.normal(ku, (D, FF), jnp.float32) * D**-0.5,
        "w_down": jax.random.normal(kd, (FF, D), jnp.float32) * FF**-0.5,
    }
    return {k: v.astype(jnp.bfloat16) for k, v in drawn.items()}


def reference(x, w_gate, w_up, w_down):
    gate = jnp.dot(x, w_gate, preferred_element_type=jnp.float32)
    up = jnp.dot(x, w_up, preferred_element_type=jnp.float32)
    hidden = (jax.nn.silu(gate) * up).astype(jnp.bfloat16)
    return jnp.dot(hidden, w_down, preferred_element_type=jnp.float32).astype(jnp.bfloat16)
```

```python
import jax
import jax.numpy as jnp
from jax import lax
from jax.experimental import pallas as pl
from jax.experimental.pallas import tpu as pltpu
from jax.sharding import PartitionSpec as P

D = 6144
F = 4096
R = 192
H2 = R // 2
NB = 512
ND = D // NB
NI = F // 512
BF = jnp.bfloat16
F32 = jnp.float32
MESH = pl.DeviceIdType.MESH
CHUNK = 48
NCH = R // CHUNK


def kernel(x_hbm, wg, wu, wd, out_hbm, X, H, W, rD, rR, rP, O, T,
           wsem, lsem, ps, pr, xs, xr, ys, yr, ds_, dr, rs, rr, qs, qr, osem):
    me = lax.axis_index("tp")
    partner = me + 1 - 2 * lax.rem(me, 2)
    remote = lax.rem(me + 2, 4)

    def rcopy(src, dst, s, r, dev):
        return pltpu.make_async_remote_copy(
            src_ref=src, dst_ref=dst, send_sem=s, recv_sem=r,
            device_id={"tp": dev}, device_id_type=MESH)

    def load_own(c):
        rows = pl.ds(c * H2, H2)
        return pltpu.make_async_copy(x_hbm.at[rows, :], X.at[rows, :], lsem.at[c])

    def to_partner(c):
        return rcopy(X.at[pl.ds(c * H2, H2), :], X.at[pl.ds(R + c * H2, H2), :],
                     ps.at[c], pr.at[c], partner)

    def far_row(k, diag):
        half, inside = (k * CHUNK) // H2, (k * CHUNK) % H2
        return 2 * R + half * R + diag * H2 + inside

    def to_remote(k):
        return rcopy(X.at[pl.ds(k * CHUNK, CHUNK), :], X.at[pl.ds(far_row(k, 0), CHUNK), :],
                     xs.at[k], xr.at[k], remote)

    def relay(k):
        return rcopy(X.at[pl.ds(far_row(k, 0), CHUNK), :], X.at[pl.ds(far_row(k, 1), CHUNK), :],
                     ys.at[k], yr.at[k], partner)

    def gu_copies(i, slot):
        out = []
        for b in range(2):
            col = pl.multiple_of(i * 512 + b * 256, 256)
            for q, w in ((0, wg), (1, wu)):
                out.append(pltpu.make_async_copy(
                    w.at[:, pl.ds(col, 256)],
                    W.at[slot, :, pl.ds(b * 512 + q * 256, 256)],
                    wsem.at[slot, 2 * b + q]))
        return out

    def dn_copy(q):
        slot = lax.rem(q + 1, 2)
        col = pl.multiple_of(lax.rem(q, ND) * NB, NB)
        return pltpu.make_async_copy(
            wd.at[:, pl.ds(col, NB)], W.at[slot, pl.ds(0, F), pl.ds(0, NB)], wsem.at[slot, 0])

    def gu(rows, m, slot, i):
        for b in range(2):
            r = jnp.dot(X[pl.ds(rows, m), :], W[slot, :, pl.ds(b * 512, 512)],
                        preferred_element_type=F32)
            col = pl.multiple_of(i * 512 + b * 256, 256)
            H[pl.ds(rows, m), pl.ds(col, 256)] = (jax.nn.silu(r[:, :256]) * r[:, 256:]).astype(BF)

    for c in range(2):
        load_own(c).start()
    for c in gu_copies(0, 0):
        c.start()

    barrier = pltpu.get_barrier_semaphore()
    for dev in (partner, remote):
        pl.semaphore_signal(barrier, inc=1, device_id={"tp": dev}, device_id_type=MESH)
    pl.semaphore_wait(barrier, 2)
    for c in range(2):
        load_own(c).wait()
        to_partner(c).start()
        for k in range(c * NCH // 2, (c + 1) * NCH // 2):
            to_remote(k).start()

    for c in gu_copies(1, 1):
        c.start()
    for c in gu_copies(0, 0):
        c.wait()
    gu(0, R, 0, 0)
    for c in range(2):
        to_partner(c).wait_recv()
    gu(R, R, 0, 0)

    def first(t, carry):
        slot = lax.rem(t, 2)
        for c in gu_copies(t, slot):
            c.wait()
        for c in gu_copies(t + 1, 1 - slot):
            c.start()

        @pl.when(t == 3)
        def _():
            to_remote(0).wait_recv()
            relay(0).start()

        gu(0, 2 * R, slot, t)
        return carry

    lax.fori_loop(1, 5, first, 0)

    def second(t, carry):
        slot = lax.rem(t, 2)
        for c in gu_copies(t, slot):
            c.wait()

        @pl.when(t < NI - 1)
        def _():
            for c in gu_copies(t + 1, 1 - slot):
                c.start()

        @pl.when(t == 5)
        def _():
            to_remote(1).wait_recv()
            relay(1).start()

        @pl.when(t == 7)
        def _():
            to_remote(2).wait_recv()
            relay(2).start()

        gu(0, 2 * R, slot, t)

        @pl.when(t == 5)
        def _():
            relay(0).wait_recv()
            relay(1).wait_recv()

        gu(2 * R, R, slot, t)
        return carry

    lax.fori_loop(5, NI, second, 0)

    to_remote(3).wait_recv()
    relay(3).start()
    relay(2).wait_recv()
    relay(3).wait_recv()

    def third(k, carry):
        i = NI - 1 - k
        slot = lax.rem(i, 2)

        @pl.when(k >= 2)
        def _():
            for c in gu_copies(i, slot):
                c.wait()

        @pl.when(k >= 1)
        def _():
            for c in gu_copies(i - 1, 1 - slot):
                c.start()

        gu(3 * R, R, slot, i)
        return carry

    lax.fori_loop(0, 3, third, 0)

    def fourth(k, carry):
        i = NI - 1 - k
        slot = lax.rem(i, 2)
        for c in gu_copies(i, slot):
            c.wait()

        @pl.when(i >= 1)
        def _():
            for c in gu_copies(i - 1, 1 - slot):
                c.start()

        @pl.when(i == 0)
        def _():
            dn_copy(0).start()

        gu(2 * R, 2 * R, slot, i)
        return carry

    lax.fori_loop(3, NI, fourth, 0)

    for c in range(2):
        to_partner(c).wait_send()
    for k in range(NCH):
        to_remote(k).wait_send()
        relay(k).wait_send()

    def cols(n):
        return pl.ds(pl.multiple_of(n * NB, NB), NB)

    def send_d(n):
        return rcopy(X.at[pl.ds(0, R), cols(n)], rD.at[:, cols(n)], ds_.at[n], dr.at[n], partner)

    def send_r(n):
        return rcopy(X.at[pl.ds(R, R), cols(n)], rR.at[:, cols(n)], rs.at[n], rr.at[n], remote)

    def send_p(n):
        return rcopy(X.at[pl.ds(2 * R, R), cols(n)], rP.at[:, cols(n)], qs.at[n], qr.at[n], partner)

    def store_out(n):
        return pltpu.make_async_copy(X.at[pl.ds(3 * R, R), cols(n)], out_hbm.at[:, cols(n)], osem.at[n])

    def pair_sum(n):
        send_d(n).wait_recv()
        X[pl.ds(R, R), cols(n)] = (
            T[lax.rem(n, 2)] + rD[:, cols(n)].astype(F32)).astype(BF)

    def far(n, carry):
        slot = lax.rem(n + 1, 2)
        dn_copy(n).wait()
        dn_copy(n + 1).start()

        @pl.when(n >= 1)
        def _():
            send_d(n - 1).start()

        @pl.when(n >= 2)
        def _():
            send_r(n - 2).start()

        r = jnp.dot(H[pl.ds(2 * R, 2 * R), :], W[slot, pl.ds(0, F), pl.ds(0, NB)],
                    preferred_element_type=F32)
        p = lax.rem(n, 2)
        for h in range(2):
            T[p, pl.ds(h * H2, H2), :] = r[h * R:h * R + H2]
            X[pl.ds(h * H2, H2), cols(n)] = r[h * R + H2:(h + 1) * R].astype(BF)

        @pl.when(n >= 1)
        def _():
            pair_sum(n - 1)

        return carry

    lax.fori_loop(0, ND, far, 0)

    def near(n, carry):
        slot = lax.rem(n + 1, 2)
        dn_copy(ND + n).wait()

        @pl.when(n < ND - 1)
        def _():
            dn_copy(ND + n + 1).start()

        @pl.when(n == 0)
        def _():
            send_d(ND - 1).start()

        @pl.when(n < 2)
        def _():
            send_r(ND - 2 + n).start()

        @pl.when(n >= 1)
        def _():
            send_p(n - 1).start()

        r = jnp.dot(H[pl.ds(0, 2 * R), :], W[slot, pl.ds(0, F), pl.ds(0, NB)],
                    preferred_element_type=F32)
        O[:, cols(n)] = r[:R]
        X[pl.ds(2 * R, R), cols(n)] = r[R:].astype(BF)

        @pl.when(n == 0)
        def _():
            pair_sum(ND - 1)

        return carry

    lax.fori_loop(0, ND, near, 0)
    send_p(ND - 1).start()

    def finish(n, carry):
        send_p(n).wait_recv()
        send_r(n).wait_recv()
        X[pl.ds(3 * R, R), cols(n)] = (
            O[:, cols(n)] + rP[:, cols(n)].astype(F32) + rR[:, cols(n)].astype(F32)).astype(BF)

        @pl.when(n >= 1)
        def _():
            store_out(n - 1).start()

        return carry

    lax.fori_loop(0, ND, finish, 0)

    def drain(n, carry):
        send_d(n).wait_send()
        send_r(n).wait_send()
        send_p(n).wait_send()
        return carry

    lax.fori_loop(0, ND, drain, 0)
    store_out(ND - 1).start()

    def stored(n, carry):
        store_out(n).wait()
        return carry

    lax.fori_loop(0, ND, stored, 0)


def solution(mesh):
    dma = pltpu.SemaphoreType.DMA

    def step(x, w_gate, w_up, w_down):
        hbm = pl.BlockSpec(memory_space=pl.ANY)
        return pl.pallas_call(
            kernel,
            out_shape=jax.ShapeDtypeStruct((R, D), BF),
            in_specs=[hbm] * 4,
            out_specs=hbm,
            scratch_shapes=[
                pltpu.VMEM((4 * R, D), BF),
                pltpu.VMEM((4 * R, F), BF),
                pltpu.VMEM((2, D, 1024), BF),
                pltpu.VMEM((R, D), BF),
                pltpu.VMEM((R, D), BF),
                pltpu.VMEM((R, D), BF),
                pltpu.VMEM((R, D), F32),
                pltpu.VMEM((2, R, NB), F32),
                dma((2, 4)), dma((2,)),
                dma((2,)), dma((2,)),
                dma((NCH,)), dma((NCH,)),
                dma((NCH,)), dma((NCH,)),
                dma((ND,)), dma((ND,)),
                dma((ND,)), dma((ND,)),
                dma((ND,)), dma((ND,)),
                dma((ND,)),
            ],
            compiler_params=pltpu.CompilerParams(
                collective_id=0, has_side_effects=True, vmem_limit_bytes=66 * 2**20 - 2**21 - 2**17),
            name="mlp",
        )(x, w_gate, w_up, w_down)

    return jax.shard_map(
        step,
        mesh=mesh,
        in_specs=(P(("dp", "tp"), None), P(None, "tp"), P(None, "tp"), P("tp", None)),
        out_specs=P(("dp", "tp"), None),
        check_vma=False,
    )
```

```python
import jax
import jax.numpy as jnp
from jax import lax
from jax.experimental import pallas as pl
from jax.experimental.pallas import tpu as pltpu
from jax.sharding import PartitionSpec as P

D = 6144
F = 4096
R = 192
KH = D // 2
NB = 512
ND = D // NB
BF = jnp.bfloat16
F32 = jnp.float32
MESH = pl.DeviceIdType.MESH
CHUNKS = ((0, 1536), (1536, 1536), (3072, 1536), (4608, 1024), (5632, 512))
NCH = len(CHUNKS)

T_K = 7
T_FAR = T_K + 8
T_LAST = T_FAR + ND
T_NEAR = T_LAST + 1
T_END = T_NEAR + ND


def kernel(x_hbm, wg, wu, wd, out, X, H, W, S, rD, rR, rP,
           wsem, lsem, ps, pr, xs, xr, ys, yr, ds_, dr, rs, rr, qs, qr):
    me = lax.axis_index("tp")
    partner = me + 1 - 2 * lax.rem(me, 2)
    remote = lax.rem(me + 2, 4)

    def rcopy(src, dst, s, r, dev):
        return pltpu.make_async_remote_copy(
            src_ref=src, dst_ref=dst, send_sem=s, recv_sem=r,
            device_id={"tp": dev}, device_id_type=MESH)

    def load_own():
        return pltpu.make_async_copy(x_hbm, X.at[pl.ds(0, R), :], lsem)

    def to_partner(c):
        rows = R // 2
        return rcopy(x_hbm.at[pl.ds(c * rows, rows), :], X.at[pl.ds(R + c * rows, rows), :],
                     ps.at[c], pr.at[c], partner)

    def to_remote(k):
        c = pl.ds(*CHUNKS[k])
        return rcopy(x_hbm.at[:, c], X.at[pl.ds(2 * R, R), c], xs.at[k], xr.at[k], remote)

    def relay(k):
        c = pl.ds(*CHUNKS[k])
        return rcopy(X.at[pl.ds(2 * R, R), c], X.at[pl.ds(3 * R, R), c], ys.at[k], yr.at[k], partner)

    def own_copies(i, slot, halves=(0, 1)):
        out = []
        for b in halves:
            col = pl.multiple_of(i * 512 + b * 256, 256)
            for q, w in ((0, wg), (1, wu)):
                out.append(pltpu.make_async_copy(
                    w.at[:, pl.ds(col, 256)],
                    W.at[slot, :, pl.ds(b * 512 + q * 256, 256)],
                    wsem.at[slot, 2 * b + q]))
        return out

    def half_copies(j, slot):
        row = pl.multiple_of((j // 4) * KH, KH)
        out = []
        for b in range(4):
            col = pl.multiple_of(lax.rem(j, 4) * 1024 + b * 256, 256)
            for q, w in ((0, wg), (1, wu)):
                out.append(pltpu.make_async_copy(
                    w.at[pl.ds(row, KH), pl.ds(col, 256)],
                    W.at[slot, pl.ds(b // 2 * KH, KH), pl.ds(b % 2 * 512 + q * 256, 256)],
                    wsem.at[slot, 2 * b + q]))
        return out

    def down_copies(n, slot):
        col = pl.multiple_of(n * NB, NB)
        return [pltpu.make_async_copy(
            wd.at[:, pl.ds(col, NB)], W.at[slot, pl.ds(0, F), pl.ds(0, NB)], wsem.at[slot, 0])]

    def own_block(t):
        return t - (T_LAST - T_K) * (t // T_LAST)

    def down_block(t):
        return t - T_FAR - (ND + 1) * (t // T_NEAR)

    is_own = lambda t: (t < T_K) | (t == T_LAST)
    is_half = lambda t: (t >= T_K) & (t < T_FAR)
    is_down = lambda t: (t >= T_FAR) & (t != T_LAST)

    def start_weights(t):
        slot = lax.rem(t, 2)

        @pl.when(is_own(t))
        def _():
            for c in own_copies(own_block(t), slot):
                c.start()

        @pl.when(is_half(t))
        def _():
            for c in half_copies(t - T_K, slot):
                c.start()

        @pl.when(is_down(t))
        def _():
            for c in down_copies(down_block(t), slot):
                c.start()

    def cols(n):
        return pl.ds(pl.multiple_of(n * NB, NB), NB)

    def hidden(i, b):
        return pl.ds(pl.multiple_of(i * 512 + b * 256, 256), 256)

    def act(r):
        return (jax.nn.silu(r[:, :256]) * r[:, 256:]).astype(BF)

    def own(rows, m, slot, i, b):
        r = jnp.dot(X[pl.ds(rows, m), :], W[slot, :, pl.ds(b * 512, 512)],
                    preferred_element_type=F32)
        H[pl.ds(rows, m), hidden(i, b)] = act(r)

    def far_half(half, slot, c, b):
        return jnp.dot(X[pl.ds(2 * R, 2 * R), pl.ds(half * KH, KH)],
                       W[slot, pl.ds(b // 2 * KH, KH), pl.ds(b % 2 * 512, 512)],
                       preferred_element_type=F32)

    def part(c, b):
        return pl.ds(pl.multiple_of(c * 2048 + b * 512, 512), 512)

    load_own().start()
    for c in own_copies(0, 0):
        c.start()

    barrier = pltpu.get_barrier_semaphore()
    for dev in (partner, remote):
        pl.semaphore_signal(barrier, inc=1, device_id={"tp": dev}, device_id_type=MESH)
    pl.semaphore_wait(barrier, 2)
    to_remote(0).start()
    for c in range(2):
        to_partner(c).start()
    for k in range(1, NCH):
        to_remote(k).start()

    for c in own_copies(1, 1):
        c.start()
    load_own().wait()
    for b in range(2):
        for c in own_copies(0, 0, (b,)):
            c.wait()
        own(0, R, 0, 0, b)
    for c in range(2):
        to_partner(c).wait_recv()
    for b in range(2):
        own(R, R, 0, 0, b)

    def send_d(n):
        return rcopy(X.at[pl.ds(2 * R, R), cols(n)], rD.at[:, cols(n)], ds_.at[n], dr.at[n], partner)

    def send_r(n):
        return rcopy(X.at[pl.ds(3 * R, R), cols(n)], rR.at[:, cols(n)], rs.at[n], rr.at[n], remote)

    def send_p(n):
        return rcopy(X.at[pl.ds(0, R), cols(n)], rP.at[:, cols(n)], qs.at[n], qr.at[n], partner)

    def held(n):
        return pl.ds(pl.multiple_of(lax.rem(n, 2) * NB, NB), NB)

    def step(t, carry):
        slot = lax.rem(t, 2)

        @pl.when(is_own(t))
        def _():
            for c in own_copies(own_block(t), slot):
                c.wait()

        @pl.when(is_half(t))
        def _():
            for c in half_copies(t - T_K, slot):
                c.wait()

        @pl.when(is_down(t))
        def _():
            for c in down_copies(down_block(t), slot):
                c.wait()

        @pl.when(t < T_END - 1)
        def _():
            start_weights(t + 1)

        for k, when in enumerate((4, 6, 9, 10, T_K + 4)):
            @pl.when(t == when)
            def _(k=k):
                to_remote(k).wait_recv()
                relay(k).start()

        @pl.when(t == T_K)
        def _():
            for k in (0, 1):
                relay(k).wait_recv()

        @pl.when(t == T_K + 4)
        def _():
            for k in (2, 3, 4):
                relay(k).wait_recv()

        @pl.when(t == T_FAR)
        def _():
            for c in range(2):
                to_partner(c).wait_send()
            for k in range(NCH):
                to_remote(k).wait_send()
                relay(k).wait_send()

        @pl.when((t > T_FAR) & (t <= T_LAST))
        def _():
            send_d(t - T_FAR - 1).start()

        @pl.when((t > T_FAR + 1) & (t <= T_NEAR))
        def _():
            send_r(t - T_FAR - 2).start()

        @pl.when(t > T_NEAR)
        def _():
            send_p(t - T_NEAR - 1).start()

        @pl.when(is_own(t))
        def _():
            for b in range(2):
                own(0, 2 * R, slot, own_block(t), b)

        @pl.when((t >= T_K) & (t < T_K + 4))
        def _():
            c = t - T_K
            for b in range(4):
                S[:, part(c, b)] = far_half(0, slot, c, b)

        @pl.when((t >= T_K + 4) & (t < T_FAR))
        def _():
            c = t - T_K - 4
            for b in range(4):
                r = far_half(1, slot, c, b) + S[:, part(c, b)]
                H[pl.ds(2 * R, 2 * R), hidden(2 * c + b // 2, b % 2)] = act(r)

        @pl.when((t >= T_FAR) & (t < T_LAST))
        def _():
            n = t - T_FAR
            r = jnp.dot(H[pl.ds(2 * R, 2 * R), :], W[slot, pl.ds(0, F), pl.ds(0, NB)],
                        preferred_element_type=F32)
            S[pl.ds(R, R), held(n)] = r[:R]
            X[pl.ds(2 * R, R), cols(n)] = r[R:].astype(BF)

        @pl.when(t >= T_NEAR)
        def _():
            n = t - T_NEAR
            r = jnp.dot(H[pl.ds(0, 2 * R), :], W[slot, pl.ds(0, F), pl.ds(0, NB)],
                        preferred_element_type=F32)
            S[pl.ds(0, R), cols(n)] = r[:R]
            X[pl.ds(0, R), cols(n)] = r[R:].astype(BF)

        @pl.when((t > T_FAR) & (t <= T_LAST))
        def _():
            n = t - T_FAR - 1
            send_d(n).wait_recv()
            X[pl.ds(3 * R, R), cols(n)] = (
                S[pl.ds(R, R), held(n)] + rD[:, cols(n)].astype(F32)).astype(BF)

        return carry

    lax.fori_loop(1, T_END, step, 0)
    send_p(ND - 1).start()

    def finish(n, carry):
        send_p(n).wait_recv()
        send_r(n).wait_recv()
        out[:, cols(n)] = (S[pl.ds(0, R), cols(n)] + rP[:, cols(n)].astype(F32)
                           + rR[:, cols(n)].astype(F32)).astype(BF)
        return carry

    lax.fori_loop(0, ND, finish, 0)

    def drain(n, carry):
        send_d(n).wait_send()
        send_r(n).wait_send()
        send_p(n).wait_send()
        return carry

    lax.fori_loop(0, ND, drain, 0)


def solution(mesh):
    dma = pltpu.SemaphoreType.DMA

    def step(x, w_gate, w_up, w_down):
        hbm = pl.BlockSpec(memory_space=pl.ANY)
        return pl.pallas_call(
            kernel,
            out_shape=pltpu.VMEM((R, D), BF),
            in_specs=[hbm] * 4,
            out_specs=pl.BlockSpec(memory_space=pltpu.VMEM),
            scratch_shapes=[
                pltpu.VMEM((4 * R, D), BF),
                pltpu.VMEM((4 * R, F), BF),
                pltpu.VMEM((2, D, 1024), BF),
                pltpu.VMEM((2 * R, 2 * F), F32),
                pltpu.VMEM((R, D), BF),
                pltpu.VMEM((R, D), BF),
                pltpu.VMEM((R, D), BF),
                dma((2, 8)), dma,
                dma((2,)), dma((2,)),
                dma((NCH,)), dma((NCH,)),
                dma((NCH,)), dma((NCH,)),
                dma((ND,)), dma((ND,)),
                dma((ND,)), dma((ND,)),
                dma((ND,)), dma((ND,)),
            ],
            compiler_params=pltpu.CompilerParams(
                collective_id=0, has_side_effects=True, vmem_limit_bytes=64500000),
            name="mlp",
        )(x, w_gate, w_up, w_down)

    return jax.shard_map(
        step,
        mesh=mesh,
        in_specs=(P(("dp", "tp"), None), P(None, "tp"), P(None, "tp"), P("tp", None)),
        out_specs=P(("dp", "tp"), None),
        check_vma=False,
    )
```

```python
import jax
import jax.numpy as jnp
from jax import lax
from jax.experimental import pallas as pl
from jax.experimental.pallas import tpu as pltpu
from jax.sharding import PartitionSpec as P

D = 6144
F = 4096
R = 192
NB = 512
ND = D // NB
BF = jnp.bfloat16
F32 = jnp.float32
MESH = pl.DeviceIdType.MESH
PART = 1536
NP = D // PART

T_P = 5
T_MID = T_P + 6
T_FAR = T_MID + 3
T_OWN = T_FAR + ND
T_NEAR = T_OWN + 2
T_END = T_NEAR + ND // 2
RELAY = (3, T_P + 1, T_P + 3, T_MID)


def kernel(x_hbm, wg, wu, wd, out, X, H, W, S, rD, rR,
           wsem, lsem, ps, pr, xs, xr, ys, yr, ds_, dr, rs, rr, qs, qr):
    me = lax.axis_index("tp")
    partner = me + 1 - 2 * lax.rem(me, 2)
    remote = lax.rem(me + 2, 4)

    def rcopy(src, dst, s, r, dev):
        return pltpu.make_async_remote_copy(
            src_ref=src, dst_ref=dst, send_sem=s, recv_sem=r,
            device_id={"tp": dev}, device_id_type=MESH)

    def load_own():
        return pltpu.make_async_copy(x_hbm, X.at[pl.ds(0, R), :], lsem)

    def to_partner(c):
        rows = R // 2
        return rcopy(x_hbm.at[pl.ds(c * rows, rows), :], X.at[pl.ds(R + c * rows, rows), :],
                     ps.at[c], pr.at[c], partner)

    def to_remote(k):
        c = pl.ds(k * PART, PART)
        return rcopy(x_hbm.at[:, c], X.at[pl.ds(2 * R, R), c], xs.at[k], xr.at[k], remote)

    def relay(k):
        c = pl.ds(k * PART, PART)
        return rcopy(X.at[pl.ds(2 * R, R), c], X.at[pl.ds(3 * R, R), c], ys.at[k], yr.at[k], partner)

    def block(i):
        return pl.ds(pl.multiple_of(i * 512, 512), 512)

    def own_copies(i, slot):
        return [pltpu.make_async_copy(
            w.at[:, pl.ds(pl.multiple_of(i * 512 + b * 256, 256), 256)],
            W.at[slot, :, pl.ds(b * 512 + q * 256, 256)], wsem.at[slot, 2 * b + q])
            for b in range(2) for q, w in ((0, wg), (1, wu))]

    def part_copies(p, slot):
        rows = pl.ds(pl.multiple_of(p // 2 * PART, PART), PART)
        return [pltpu.make_async_copy(
            w.at[rows, block(p % 2 * 4 + e)],
            W.at[slot, pl.ds(e * PART, PART), pl.ds(q * 512, 512)], wsem.at[slot, 2 * e + q])
            for e in range(4) for q, w in ((0, wg), (1, wu))]

    def down_copy(pair, slot):
        c = pl.ds(pl.multiple_of(pair * 1024, 1024), 1024)
        return pltpu.make_async_copy(wd.at[:, c], W.at[slot, pl.ds(0, F), :], wsem.at[slot, 0])

    def own_block(t):
        return t - 6 * (t // T_MID) - (T_OWN - T_MID - 1) * (t // T_OWN) + 6 * (t // (2 * T_MID))

    def part_step(t):
        return t - T_P - t // (T_MID + 1)

    def cols(n):
        return pl.ds(pl.multiple_of(n * NB, NB), NB)

    def wide(n):
        return pl.ds(pl.multiple_of(n * 1024, 1024), 1024)

    def dot(a, w):
        return jnp.dot(a, w, preferred_element_type=F32)

    def own(rows, m, slot, i):
        for b in range(2):
            r = dot(X[pl.ds(rows, m), :], W[slot, :, pl.ds(b * 512, 512)])
            c = pl.ds(pl.multiple_of(i * 512 + b * 256, 256), 256)
            H[pl.ds(rows, m), c] = (jax.nn.silu(r[:, :256]) * r[:, 256:]).astype(BF)

    def part(slot, p, e, q):
        x = X[pl.ds(2 * R, 2 * R), pl.ds(pl.multiple_of(p // 2 * PART, PART), PART)]
        c = block((p % 2 * 4 + e) * 2 + q)
        return c, dot(x, W[slot, pl.ds(e * PART, PART), pl.ds(q * 512, 512)]) + S[:, c]

    load_own().start()
    for c in own_copies(0, 0):
        c.start()

    barrier = pltpu.get_barrier_semaphore()
    for dev in (partner, remote):
        pl.semaphore_signal(barrier, inc=1, device_id={"tp": dev}, device_id_type=MESH)
    pl.semaphore_wait(barrier, 2)
    to_remote(0).start()
    for c in range(2):
        to_partner(c).start()
    for k in range(1, NP):
        to_remote(k).start()
    for c in own_copies(1, 1):
        c.start()

    def clear(k, carry):
        S[pl.ds(pl.multiple_of(k * 8, 8), 8), :] = jnp.zeros((8, 2 * F), F32)
        return carry

    lax.fori_loop(0, 2 * R // 8, clear, 0)
    load_own().wait()
    for c in own_copies(0, 0):
        c.wait()
    own(0, R, 0, 0)
    for c in range(2):
        to_partner(c).wait_recv()
    own(R, R, 0, 0)

    def send_d(n):
        return rcopy(X.at[pl.ds(2 * R, R), cols(n)], rD.at[:, cols(n)], ds_.at[n], dr.at[n], partner)

    def send_r(n):
        return rcopy(X.at[pl.ds(3 * R, R), cols(n)], rR.at[:, cols(n)], rs.at[n], rr.at[n], remote)

    def landing(n):
        return pl.ds(pl.multiple_of(2 * R + lax.rem(n, 2) * R, 64), R)

    def send_p(n):
        return rcopy(X.at[pl.ds(0, R), wide(n)], H.at[landing(n), wide(n // 2)], qs.at[n], qr.at[n], partner)

    def held(n):
        return pl.ds(pl.multiple_of(lax.rem(n, 2) * NB, NB), NB)

    def prefetch_up(t):
        slot = lax.rem(t, 2)

        @pl.when((t < T_P) | (t == T_MID))
        def _():
            for c in own_copies(own_block(t), slot):
                c.start()

        @pl.when((t >= T_P) & (t < T_FAR) & (t != T_MID))
        def _():
            for c in part_copies(part_step(t), slot):
                c.start()

        @pl.when(t == T_FAR)
        def _():
            down_copy(0, slot).start()

    def wait_own(t, slot):
        for c in own_copies(own_block(t), slot):
            c.wait()

    def step(t, carry):
        slot = lax.rem(t, 2)

        @pl.when(t < T_FAR)
        def _():
            prefetch_up(t + 1)
            for k in range(NP):
                @pl.when(t == RELAY[k])
                def _(k=k):
                    to_remote(k).wait_recv()
                    relay(k).start()

            @pl.when((t >= T_P) & (t != T_MID))
            def _():
                p = part_step(t)
                for k in range(NP):
                    @pl.when(p == 2 * k)
                    def _(k=k):
                        relay(k).wait_recv()
                for c in part_copies(p, slot):
                    c.wait()

                @pl.when(t < T_MID)
                def _():
                    for e in range(4):
                        for q in range(2):
                            c, r = part(slot, p, e, q)
                            S[:, c] = r

                @pl.when(t > T_MID)
                def _():
                    for e in range(4):
                        c, r = part(slot, p, e, 0)
                        S[:, c] = jax.nn.silu(r)
                        up = part(slot, p, e, 1)[1]
                        H[pl.ds(2 * R, 2 * R), block(p % 2 * 4 + e)] = (S[:, c] * up).astype(BF)

        @pl.when((t >= T_FAR) & (t < T_NEAR))
        def _():
            n = t - T_FAR
            pair = n // 2

            @pl.when((lax.rem(n, 2) == 0) & (n < ND - 2))
            def _():
                down_copy(pair + 1, lax.rem(pair + 1, 2)).start()

            @pl.when((n == ND - 2) | (n == ND))
            def _():
                for c in own_copies(pair - ND // 2 + 7, lax.rem(pair + 1, 2)):
                    c.start()

            @pl.when(n == ND + 1)
            def _():
                down_copy(0, 0).start()

            @pl.when(n == 0)
            def _():
                for c in range(2):
                    to_partner(c).wait_send()
                for k in range(NP):
                    to_remote(k).wait_send()
                    relay(k).wait_send()

            @pl.when((n > 0) & (n <= ND))
            def _():
                send_d(n - 1).start()

            @pl.when(n > 1)
            def _():
                send_r(n - 2).start()

        @pl.when((t < T_P) | (t == T_MID) | ((t >= T_OWN) & (t < T_NEAR)))
        def _():
            wait_own(t, slot)
            own(0, 2 * R, slot, own_block(t))

        @pl.when((t >= T_FAR) & (t < T_OWN))
        def _():
            n = t - T_FAR
            s = lax.rem(n // 2, 2)

            @pl.when(lax.rem(n, 2) == 0)
            def _():
                down_copy(n // 2, s).wait()

            r = dot(H[pl.ds(2 * R, 2 * R), :], W[s, pl.ds(0, F), held(n)])
            S[pl.ds(R, R), held(n)] = r[:R]
            X[pl.ds(2 * R, R), cols(n)] = r[R:].astype(BF)

        @pl.when((t > T_FAR) & (t <= T_OWN))
        def _():
            n = t - T_FAR - 1
            send_d(n).wait_recv()
            X[pl.ds(3 * R, R), cols(n)] = (
                S[pl.ds(R, R), held(n)] + rD[:, cols(n)].astype(F32)).astype(BF)

        @pl.when(t >= T_NEAR)
        def _():
            m = t - T_NEAR

            @pl.when(m < ND // 2 - 1)
            def _():
                down_copy(m + 1, 1 - slot).start()

            @pl.when(m > 0)
            def _():
                send_p(m - 1).start()

            down_copy(m, slot).wait()
            for b in range(2):
                r = dot(H[pl.ds(0, 2 * R), :], W[slot, pl.ds(0, F), pl.ds(b * NB, NB)])
                c = cols(2 * m + b)
                S[pl.ds(0, R), c] = r[:R]
                X[pl.ds(0, R), c] = r[R:].astype(BF)

        return carry

    lax.fori_loop(1, T_END, step, 0)
    send_p(ND // 2 - 1).start()

    def finish(n, carry):
        @pl.when(lax.rem(n, 2) == 0)
        def _():
            send_p(n // 2).wait_recv()
        send_r(n).wait_recv()
        near = H[landing(n // 2), cols(n // 4 * 2 + lax.rem(n, 2))]
        out[:, cols(n)] = (S[pl.ds(0, R), cols(n)] + near.astype(F32)
                           + rR[:, cols(n)].astype(F32)).astype(BF)
        return carry

    lax.fori_loop(0, ND, finish, 0)

    def drain(n, carry):
        send_d(n).wait_send()
        send_r(n).wait_send()
        return carry

    lax.fori_loop(0, ND, drain, 0)
    for n in range(ND // 2):
        send_p(n).wait_send()


def solution(mesh):
    dma = pltpu.SemaphoreType.DMA

    def step(x, w_gate, w_up, w_down):
        hbm = pl.BlockSpec(memory_space=pl.ANY)
        return pl.pallas_call(
            kernel,
            out_shape=pltpu.VMEM((R, D), BF),
            in_specs=[hbm] * 4,
            out_specs=pl.BlockSpec(memory_space=pltpu.VMEM),
            scratch_shapes=[
                pltpu.VMEM((4 * R, D), BF),
                pltpu.VMEM((4 * R, F), BF),
                pltpu.VMEM((2, D, 1024), BF),
                pltpu.VMEM((2 * R, 2 * F), F32),
                pltpu.VMEM((R, D), BF),
                pltpu.VMEM((R, D), BF),
                dma((2, 8)), dma,
                dma((2,)), dma((2,)),
                dma((NP,)), dma((NP,)),
                dma((NP,)), dma((NP,)),
                dma((ND,)), dma((ND,)),
                dma((ND,)), dma((ND,)),
                dma((ND // 2,)), dma((ND // 2,)),
            ],
            compiler_params=pltpu.CompilerParams(
                collective_id=0, has_side_effects=True, vmem_limit_bytes=64500000),
            name="mlp",
        )(x, w_gate, w_up, w_down)

    return jax.shard_map(
        step,
        mesh=mesh,
        in_specs=(P(("dp", "tp"), None), P(None, "tp"), P(None, "tp"), P("tp", None)),
        out_specs=P(("dp", "tp"), None),
        check_vma=False,
    )
```

```python
import jax
import jax.numpy as jnp
from jax import lax
from jax.experimental import pallas as pl
from jax.experimental.pallas import tpu as pltpu
from jax.sharding import PartitionSpec as P

D = 6144
F = 4096
R = 192
NB = 512
ND = D // NB
BF = jnp.bfloat16
F32 = jnp.float32
MESH = pl.DeviceIdType.MESH
PART = 1536
NP = D // PART

T_P = 5
T_FAR = T_P + 2 * NP
T_OWN = T_FAR + ND // 2 + 1
T_NEAR = T_OWN + 3
T_END = T_NEAR + ND // 2
RELAY = (3, T_P + 1, T_P + 3, T_P + 5)
NU = ND // 2 + 1


def kernel(x_hbm, wg, wu, wd, out, X, H, W, S, rD, rR,
           wsem, lsem, ps, pr, xs, xr, ys, yr, ds_, dr, rs, rr, qs, qr):
    me = lax.axis_index("tp")
    partner = me + 1 - 2 * lax.rem(me, 2)
    remote = lax.rem(me + 2, 4)

    def rcopy(src, dst, s, r, dev):
        return pltpu.make_async_remote_copy(
            src_ref=src, dst_ref=dst, send_sem=s, recv_sem=r,
            device_id={"tp": dev}, device_id_type=MESH)

    def load_own():
        return pltpu.make_async_copy(x_hbm, X.at[pl.ds(0, R), :], lsem)

    def to_partner(c):
        rows = R // 2
        return rcopy(x_hbm.at[pl.ds(c * rows, rows), :], X.at[pl.ds(R + c * rows, rows), :],
                     ps.at[c], pr.at[c], partner)

    def to_remote(k):
        c = pl.ds(k * PART, PART)
        return rcopy(x_hbm.at[:, c], X.at[pl.ds(2 * R, R), c], xs.at[k], xr.at[k], remote)

    def relay(k):
        c = pl.ds(k * PART, PART)
        return rcopy(X.at[pl.ds(2 * R, R), c], X.at[pl.ds(3 * R, R), c], ys.at[k], yr.at[k], partner)

    def block(i):
        return pl.ds(pl.multiple_of(i * 512, 512), 512)

    def own_copies(i, slot, halves=(0, 1)):
        return [pltpu.make_async_copy(
            w.at[:, pl.ds(pl.multiple_of(i * 512 + b * 256, 256), 256)],
            W.at[slot, :, pl.ds(b * 512 + q * 256, 256)], wsem.at[slot, 2 * b + q])
            for b in halves for q, w in ((0, wg), (1, wu))]

    def part_copies(p, slot):
        rows = pl.ds(pl.multiple_of(p // 2 * PART, PART), PART)
        return [pltpu.make_async_copy(
            w.at[rows, block(p % 2 * 4 + e)],
            W.at[slot, pl.ds(e * PART, PART), pl.ds(q * 512, 512)], wsem.at[slot, 2 * e + q])
            for e in range(4) for q, w in ((0, wg), (1, wu))]

    def down_copy(pair, slot):
        c = pl.ds(pl.multiple_of(pair * 1024, 1024), 1024)
        return pltpu.make_async_copy(wd.at[:, c], W.at[slot, pl.ds(0, F), :], wsem.at[slot, 0])

    def own_block(t):
        return t - (T_OWN - T_P) * (t // T_OWN)

    def cols(n):
        return pl.ds(pl.multiple_of(n * NB, NB), NB)

    def wide(n):
        return pl.ds(pl.multiple_of(n * 1024, 1024), 1024)

    def dot(a, w):
        return jnp.dot(a, w, preferred_element_type=F32)

    def own(rows, m, slot, i, halves=(0, 1)):
        for b in halves:
            r = dot(X[pl.ds(rows, m), :], W[slot, :, pl.ds(b * 512, 512)])
            c = pl.ds(pl.multiple_of(i * 512 + b * 256, 256), 256)
            H[pl.ds(rows, m), c] = (jax.nn.silu(r[:, :256]) * r[:, 256:]).astype(BF)

    def part(slot, p, e, q):
        x = X[pl.ds(2 * R, 2 * R), pl.ds(pl.multiple_of(p // 2 * PART, PART), PART)]
        c = block((p % 2 * 4 + e) * 2 + q)
        return c, dot(x, W[slot, pl.ds(e * PART, PART), pl.ds(q * 512, 512)]) + S[:, c]

    load_own().start()
    for c in own_copies(0, 0, (0,)):
        c.start()

    barrier = pltpu.get_barrier_semaphore()
    for dev in (partner, remote):
        pl.semaphore_signal(barrier, inc=1, device_id={"tp": dev}, device_id_type=MESH)

    def clear(k, carry):
        S[pl.ds(pl.multiple_of(k * 8, 8), 8), :] = jnp.zeros((8, 2 * F), F32)
        return carry

    lax.fori_loop(0, 2 * R // 8, clear, 0)
    pl.semaphore_wait(barrier, 2)
    to_remote(0).start()
    for c in range(2):
        to_partner(c).start()
    for k in range(1, NP):
        to_remote(k).start()
    for c in own_copies(0, 0, (1,)) + own_copies(1, 1):
        c.start()
    load_own().wait()
    for b in range(2):
        for c in own_copies(0, 0, (b,)):
            c.wait()
        own(0, R, 0, 0, (b,))
    for c in range(2):
        to_partner(c).wait_recv()
    own(R, R, 0, 0)

    def far_copy(u, rows, dst, s, r, dev, go):
        @pl.when(u < 2)
        def _():
            c = cols(u)
            go(rcopy(X.at[rows, c], dst.at[:, c], s.at[u], r.at[u], dev))

        @pl.when(u >= 2)
        def _():
            c = wide(u - 1)
            go(rcopy(X.at[rows, c], dst.at[:, c], s.at[u], r.at[u], dev))

    def send_d(u, go):
        far_copy(u, pl.ds(2 * R, R), rD, ds_, dr, partner, go)

    def send_r(u, go):
        far_copy(u, pl.ds(3 * R, R), rR, rs, rr, remote, go)

    start = lambda c: c.start()
    wait_send = lambda c: c.wait_send()
    wait_recv = lambda c: c.wait_recv()

    def landing(n):
        return pl.ds(pl.multiple_of(2 * R + lax.rem(n, 2) * R, 64), R)

    def send_p(n):
        return rcopy(X.at[pl.ds(0, R), wide(n)], H.at[landing(n), wide(n // 2)], qs.at[n], qr.at[n], partner)

    def pair_sum(c, h):
        X[pl.ds(3 * R, R), c] = (S[pl.ds(R, R), h] + rD[:, c].astype(F32)).astype(BF)

    def down(rows, slot, w, keep_rows, keep, send_rows, c):
        r = dot(H[pl.ds(rows, 2 * R), :], W[slot, pl.ds(0, F), w])
        S[keep_rows, keep] = r[:R]
        X[send_rows, c] = r[R:].astype(BF)

    def step(t, carry):
        late = t // (T_FAR + 1) - t // (2 * T_FAR + 2)
        slot = lax.rem(t + late, 2)
        other = 1 - slot

        @pl.when(t < T_FAR)
        def _():
            @pl.when(t < T_P - 1)
            def _():
                for c in own_copies(t + 1, other):
                    c.start()

            @pl.when((t >= T_P - 1) & (t < T_FAR - 1))
            def _():
                for c in part_copies(t + 1 - T_P, other):
                    c.start()

            @pl.when(t == T_FAR - 1)
            def _():
                down_copy(0, other).start()

            @pl.when((t == RELAY[0]) | (t == RELAY[1]) | (t == RELAY[2]) | (t == RELAY[3]))
            def _():
                for k in range(NP):
                    @pl.when(t == RELAY[k])
                    def _(k=k):
                        to_remote(k).wait_recv()
                        relay(k).start()

            @pl.when(t >= T_P)
            def _():
                p = t - T_P

                @pl.when(lax.rem(p, 2) == 0)
                def _():
                    for k in range(NP):
                        @pl.when(p == 2 * k)
                        def _(k=k):
                            relay(k).wait_recv()

                for c in part_copies(p, slot):
                    c.wait()

                @pl.when(p < 2 * NP - 2)
                def _():
                    for e in range(4):
                        for q in range(2):
                            c, r = part(slot, p, e, q)
                            S[:, c] = r

                @pl.when(p >= 2 * NP - 2)
                def _():
                    for e in range(4):
                        c, r = part(slot, p, e, 0)
                        S[:, c] = jax.nn.silu(r)
                        up = part(slot, p, e, 1)[1]
                        H[pl.ds(2 * R, 2 * R), block(lax.rem(p, 2) * 4 + e)] = (S[:, c] * up).astype(BF)

        @pl.when((t >= T_FAR) & (t < T_NEAR))
        def _():
            u = t - T_FAR

            @pl.when(u == 0)
            def _():
                down_copy(1, other).start()
                for c in range(2):
                    to_partner(c).wait_send()
                for k in range(NP):
                    to_remote(k).wait_send()
                    relay(k).wait_send()

            @pl.when((u > 1) & (u < NU - 1))
            def _():
                down_copy(u, other).start()

            @pl.when((u >= NU - 1) & (u < NU + 2))
            def _():
                for c in own_copies(T_P + u - NU + 1, other):
                    c.start()

            @pl.when(u == NU + 2)
            def _():
                down_copy(0, other).start()

            @pl.when((u > 0) & (u <= NU))
            def _():
                send_d(u - 1, start)

            @pl.when((u > 1) & (u <= NU + 1))
            def _():
                send_r(u - 2, start)

            @pl.when(u < 2)
            def _():
                @pl.when(u == 0)
                def _():
                    down_copy(0, T_FAR % 2).wait()

                down(2 * R, T_FAR % 2, cols(u), pl.ds(R, R), cols(u), pl.ds(2 * R, R), cols(u))

        @pl.when((t < T_P) | ((t >= T_OWN) & (t < T_NEAR)))
        def _():
            i = own_block(t)
            for c in own_copies(i, slot):
                c.wait()
            own(0, 2 * R, slot, i)

        @pl.when(((t >= T_FAR + 2) & (t < T_OWN)) | (t >= T_NEAR))
        def _():
            near = t // T_NEAR
            m = t - T_FAR - 1 - (T_NEAR - T_FAR - 1) * near

            @pl.when((t >= T_NEAR) & (m < ND // 2 - 1))
            def _():
                down_copy(m + 1, other).start()

            @pl.when((t >= T_NEAR) & (m > 0))
            def _():
                send_p(m - 1).start()

            down_copy(m, slot).wait()
            far = 1 - near
            k = 2 * (lax.rem(m, 2) * far + m * near)
            for b in range(2):
                down(pl.multiple_of(2 * R * far, 128), slot, pl.ds(b * NB, NB),
                     pl.ds(pl.multiple_of(R * far, 64), R), cols(k + b),
                     pl.ds(pl.multiple_of(2 * R * far, 128), R), cols(2 * m + b))

        @pl.when((t > T_FAR) & (t <= T_OWN))
        def _():
            u = t - T_FAR - 1
            send_d(u, wait_recv)

            @pl.when(u < 2)
            def _():
                pair_sum(cols(u), cols(u))

            @pl.when(u >= 2)
            def _():
                pair_sum(wide(u - 1), wide(lax.rem(u - 1, 2)))

        return carry

    lax.fori_loop(1, T_END, step, 0)
    send_p(ND // 2 - 1).start()

    def finish(n, carry):
        send_p(n).wait_recv()

        @pl.when(n == 0)
        def _():
            send_r(0, wait_recv)

        send_r(n + 1, wait_recv)
        out[:, wide(n)] = (S[pl.ds(0, R), wide(n)] + H[landing(n), wide(n // 2)].astype(F32)
                           + rR[:, wide(n)].astype(F32)).astype(BF)
        return carry

    lax.fori_loop(0, ND // 2, finish, 0)

    def drain(u, carry):
        send_d(u, wait_send)
        send_r(u, wait_send)
        return carry

    lax.fori_loop(0, NU, drain, 0)
    for n in range(ND // 2):
        send_p(n).wait_send()


def solution(mesh):
    dma = pltpu.SemaphoreType.DMA

    def step(x, w_gate, w_up, w_down):
        hbm = pl.BlockSpec(memory_space=pl.ANY)
        return pl.pallas_call(
            kernel,
            out_shape=pltpu.VMEM((R, D), BF),
            in_specs=[hbm] * 4,
            out_specs=pl.BlockSpec(memory_space=pltpu.VMEM),
            scratch_shapes=[
                pltpu.VMEM((4 * R, D), BF),
                pltpu.VMEM((4 * R, F), BF),
                pltpu.VMEM((2, D, 1024), BF),
                pltpu.VMEM((2 * R, 2 * F), F32),
                pltpu.VMEM((R, D), BF),
                pltpu.VMEM((R, D), BF),
                dma((2, 8)), dma,
                dma((2,)), dma((2,)),
                dma((NP,)), dma((NP,)),
                dma((NP,)), dma((NP,)),
                dma((NU,)), dma((NU,)),
                dma((NU,)), dma((NU,)),
                dma((ND // 2,)), dma((ND // 2,)),
            ],
            compiler_params=pltpu.CompilerParams(
                collective_id=0, has_side_effects=True, vmem_limit_bytes=64500000),
            name="mlp",
        )(x, w_gate, w_up, w_down)

    return jax.shard_map(
        step,
        mesh=mesh,
        in_specs=(P(("dp", "tp"), None), P(None, "tp"), P(None, "tp"), P("tp", None)),
        out_specs=P(("dp", "tp"), None),
        check_vma=False,
    )
```

```python
import jax
import jax.numpy as jnp
from jax import lax
from jax.experimental import pallas as pl
from jax.experimental.pallas import tpu as pltpu
from jax.sharding import PartitionSpec as P

D = 6144
F = 4096
R = 192
NB = 512
ND = D // NB
BF = jnp.bfloat16
F32 = jnp.float32
MESH = pl.DeviceIdType.MESH
PART = 1536
NP = D // PART

T_P = 5
T_FAR = T_P + 2 * NP
T_OWN = T_FAR + ND // 2 + 1
T_NEAR = T_OWN + 3
T_END = T_NEAR + ND // 2 - 1
RELAY = (3, T_P + 1, T_P + 3, T_P + 5)
NU = ND // 2 + 1


def kernel(x_hbm, wg, wu, wd, out, X, H, W, S, rD, rR,
           wsem, lsem, ps, pr, xs, xr, ys, yr, ds_, dr, rs, rr, qs, qr):
    me = lax.axis_index("tp")
    partner = me + 1 - 2 * lax.rem(me, 2)
    remote = lax.rem(me + 2, 4)

    def rcopy(src, dst, s, r, dev):
        return pltpu.make_async_remote_copy(
            src_ref=src, dst_ref=dst, send_sem=s, recv_sem=r,
            device_id={"tp": dev}, device_id_type=MESH)

    def load_own():
        return pltpu.make_async_copy(x_hbm, X.at[pl.ds(0, R), :], lsem)

    def to_partner(c):
        rows = R // 2
        return rcopy(x_hbm.at[pl.ds(c * rows, rows), :], X.at[pl.ds(R + c * rows, rows), :],
                     ps.at[c], pr.at[c], partner)

    def to_remote(k):
        c = pl.ds(k * PART, PART)
        return rcopy(x_hbm.at[:, c], X.at[pl.ds(2 * R, R), c], xs.at[k], xr.at[k], remote)

    def relay(k):
        c = pl.ds(k * PART, PART)
        return rcopy(X.at[pl.ds(2 * R, R), c], X.at[pl.ds(3 * R, R), c], ys.at[k], yr.at[k], partner)

    def block(i):
        return pl.ds(pl.multiple_of(i * 512, 512), 512)

    def own_copies(i, slot, halves=(0, 1), rows=pl.ds(0, D)):
        return [pltpu.make_async_copy(
            w.at[rows, pl.ds(pl.multiple_of(i * 512 + b * 256, 256), 256)],
            W.at[slot, rows, pl.ds(b * 512 + q * 256, 256)], wsem.at[slot, 2 * b + q])
            for b in halves for q, w in ((0, wg), (1, wu))]

    def part_copies(p, slot):
        rows = pl.ds(pl.multiple_of(p // 2 * PART, PART), PART)
        return [pltpu.make_async_copy(
            w.at[rows, block(p % 2 * 4 + e)],
            W.at[slot, pl.ds(e * PART, PART), pl.ds(q * 512, 512)], wsem.at[slot, 2 * e + q])
            for e in range(4) for q, w in ((0, wg), (1, wu))]

    def down_copy(pair, slot):
        c = pl.ds(pl.multiple_of(pair * 1024, 1024), 1024)
        return pltpu.make_async_copy(wd.at[:, c], W.at[slot, pl.ds(0, F), :], wsem.at[slot, 7])

    def own_block(t):
        return t - (T_OWN - T_P) * (t // T_OWN)

    def at(start, size):
        return pl.ds(start if isinstance(start, int) else pl.multiple_of(start, size), size)

    def cols(n):
        return at(n * NB, NB)

    def wide(n):
        return at(n * 1024, 1024)

    def dot(a, w):
        return jnp.dot(a, w, preferred_element_type=F32)

    def own(rows, m, slot, i, halves=(0, 1)):
        for b in halves:
            r = dot(X[pl.ds(rows, m), :], W[slot, :, pl.ds(b * 512, 512)])
            c = pl.ds(pl.multiple_of(i * 512 + b * 256, 256), 256)
            H[pl.ds(rows, m), c] = (jax.nn.silu(r[:, :256]) * r[:, 256:]).astype(BF)

    def part(slot, p, e, q):
        x = X[pl.ds(2 * R, 2 * R), pl.ds(pl.multiple_of(p // 2 * PART, PART), PART)]
        c = block((p % 2 * 4 + e) * 2 + q)
        return c, dot(x, W[slot, pl.ds(e * PART, PART), pl.ds(q * 512, 512)]) + S[:, c]

    load_own().start()
    for c in own_copies(0, 0, (0,)):
        c.start()

    barrier = pltpu.get_barrier_semaphore()
    for dev in (partner, remote):
        pl.semaphore_signal(barrier, inc=1, device_id={"tp": dev}, device_id_type=MESH)

    def clear(k, carry):
        S[pl.ds(pl.multiple_of(k * 8, 8), 8), :] = jnp.zeros((8, 2 * F), F32)
        return carry

    lax.fori_loop(0, 2 * R // 8, clear, 0)
    for c in own_copies(0, 0, (1,)):
        c.start()
    pl.semaphore_wait(barrier, 2)
    to_remote(0).start()
    for c in range(2):
        to_partner(c).start()
    for k in range(1, NP):
        to_remote(k).start()
    for c in own_copies(1, 1):
        c.start()
    load_own().wait()
    for b in range(2):
        for c in own_copies(0, 0, (b,)):
            c.wait()
        own(0, R, 0, 0, (b,))
    for c in range(2):
        to_partner(c).wait_recv()
    own(R, R, 0, 0)

    def far_copy(u, rows, dst, s, r, dev, go):
        if isinstance(u, int):
            c = cols(u) if u < 2 else wide(u - 1)
            go(rcopy(X.at[rows, c], dst.at[:, c], s.at[u], r.at[u], dev))
            return

        @pl.when(u < 2)
        def _():
            c = cols(u)
            go(rcopy(X.at[rows, c], dst.at[:, c], s.at[u], r.at[u], dev))

        @pl.when(u >= 2)
        def _():
            c = wide(u - 1)
            go(rcopy(X.at[rows, c], dst.at[:, c], s.at[u], r.at[u], dev))

    def send_d(u, go):
        far_copy(u, pl.ds(2 * R, R), rD, ds_, dr, partner, go)

    def send_r(u, go):
        far_copy(u, pl.ds(3 * R, R), rR, rs, rr, remote, go)

    start = lambda c: c.start()
    wait_send = lambda c: c.wait_send()
    wait_recv = lambda c: c.wait_recv()

    def landing(n):
        return pl.ds(2 * R + n % 2 * R, R)

    def send_p(n):
        return rcopy(X.at[pl.ds(0, R), wide(n)], H.at[landing(n), wide(n // 2)], qs.at[n], qr.at[n], partner)

    def pair_sum(c, h):
        X[pl.ds(3 * R, R), c] = (S[pl.ds(R, R), h] + rD[:, c].astype(F32)).astype(BF)

    def down(rows, slot, w, keep_rows, keep, send_rows, c):
        r = dot(H[pl.ds(rows, 2 * R), :], W[slot, pl.ds(0, F), w])
        S[keep_rows, keep] = r[:R]
        X[send_rows, c] = r[R:].astype(BF)

    def step(t, carry):
        late = t // (T_FAR + 1) - t // (2 * T_FAR + 2)
        slot = lax.rem(t + late, 2)
        other = 1 - slot

        @pl.when(t < T_FAR)
        def _():
            @pl.when(t < T_P - 1)
            def _():
                for c in own_copies(t + 1, other):
                    c.start()

            @pl.when((t >= T_P - 1) & (t < T_FAR - 1))
            def _():
                for c in part_copies(t + 1 - T_P, other):
                    c.start()

            @pl.when(t == T_FAR - 1)
            def _():
                down_copy(0, other).start()

            @pl.when((t == RELAY[0]) | (t == RELAY[1]) | (t == RELAY[2]) | (t == RELAY[3]))
            def _():
                for k in range(NP):
                    @pl.when(t == RELAY[k])
                    def _(k=k):
                        to_remote(k).wait_recv()
                        relay(k).start()

            @pl.when(t >= T_P)
            def _():
                p = t - T_P

                @pl.when(lax.rem(p, 2) == 0)
                def _():
                    for k in range(NP):
                        @pl.when(p == 2 * k)
                        def _(k=k):
                            relay(k).wait_recv()

                for c in part_copies(p, slot):
                    c.wait()

                @pl.when(p < 2 * NP - 2)
                def _():
                    for e in range(4):
                        for q in range(2):
                            c, r = part(slot, p, e, q)
                            S[:, c] = r

                @pl.when(p >= 2 * NP - 2)
                def _():
                    for e in range(4):
                        c, r = part(slot, p, e, 0)
                        S[:, c] = jax.nn.silu(r)
                        up = part(slot, p, e, 1)[1]
                        H[pl.ds(2 * R, 2 * R), block(lax.rem(p, 2) * 4 + e)] = (S[:, c] * up).astype(BF)

        @pl.when((t >= T_FAR) & (t < T_NEAR))
        def _():
            u = t - T_FAR

            @pl.when(u == 0)
            def _():
                down_copy(1, other).start()
                for c in range(2):
                    to_partner(c).wait_send()
                for k in range(NP):
                    to_remote(k).wait_send()
                    relay(k).wait_send()

            @pl.when((u > 1) & (u < NU - 1))
            def _():
                down_copy(u, other).start()

            @pl.when(u == NU - 2)
            def _():
                for c in own_copies(T_P, slot, rows=pl.ds(F, D - F)):
                    c.start()

            @pl.when(u == NU - 1)
            def _():
                for c in own_copies(T_P, other, rows=pl.ds(0, F)):
                    c.start()

            @pl.when((u >= NU) & (u < NU + 2))
            def _():
                for c in own_copies(T_P + u - NU + 1, other):
                    c.start()

            @pl.when(u == NU + 2)
            def _():
                down_copy(0, other).start()

            @pl.when((u > 0) & (u <= NU))
            def _():
                send_d(u - 1, start)

            @pl.when((u > 1) & (u <= NU + 1))
            def _():
                send_r(u - 2, start)

            @pl.when(u < 2)
            def _():
                @pl.when(u == 0)
                def _():
                    down_copy(0, T_FAR % 2).wait()

                down(2 * R, T_FAR % 2, cols(u), pl.ds(R, R), cols(u), pl.ds(2 * R, R), cols(u))

        @pl.when((t < T_P) | ((t >= T_OWN) & (t < T_NEAR)))
        def _():
            i = own_block(t)
            for c in own_copies(i, slot):
                c.wait()
            own(0, 2 * R, slot, i)

        @pl.when(((t >= T_FAR + 2) & (t < T_OWN)) | (t >= T_NEAR))
        def _():
            near = t // T_NEAR
            m = t - T_FAR - 1 - (T_NEAR - T_FAR - 1) * near

            @pl.when(t >= T_NEAR)
            def _():
                down_copy(m + 1, other).start()

            @pl.when((t >= T_NEAR) & (m > 0))
            def _():
                send_p(m - 1).start()

            down_copy(m, slot).wait()
            far = 1 - near
            k = 2 * (lax.rem(m, 2) * far + m * near)
            for b in range(2):
                down(pl.multiple_of(2 * R * far, 128), slot, pl.ds(b * NB, NB),
                     pl.ds(pl.multiple_of(R * far, 64), R), cols(k + b),
                     pl.ds(pl.multiple_of(2 * R * far, 128), R), cols(2 * m + b))

        @pl.when((t > T_FAR) & (t <= T_OWN))
        def _():
            u = t - T_FAR - 1
            send_d(u, wait_recv)

            @pl.when(u < 2)
            def _():
                pair_sum(cols(u), cols(u))

            @pl.when(u >= 2)
            def _():
                pair_sum(wide(u - 1), wide(lax.rem(u - 1, 2)))

        return carry

    lax.fori_loop(1, T_END, step, 0)

    last = ND // 2 - 1

    def arrived(n):
        send_p(n).wait_recv()
        if n == 0:
            send_r(0, wait_recv)
        send_r(n + 1, wait_recv)

    def finish(n):
        out[:, wide(n)] = (S[pl.ds(0, R), wide(n)] + H[landing(n), wide(n // 2)].astype(F32)
                           + rR[:, wide(n)].astype(F32)).astype(BF)

    def last_dot(rows, b):
        return dot(H[pl.ds(rows, R), :], W[(T_END + 1) % 2, pl.ds(0, F), pl.ds(b * NB, NB)])

    send_p(last - 1).start()
    down_copy(last, (T_END + 1) % 2).wait()
    for b in range(2):
        X[pl.ds(0, R), cols(2 * last + b)] = last_dot(R, b).astype(BF)
    send_p(last).start()
    for b in range(2):
        S[pl.ds(0, R), cols(2 * last + b)] = last_dot(0, b)
    for n in range(last + 1):
        arrived(n)
        finish(n)

    def drain(u, carry):
        send_d(u, wait_send)
        send_r(u, wait_send)
        return carry

    lax.fori_loop(0, NU, drain, 0)
    for n in range(ND // 2):
        send_p(n).wait_send()


def solution(mesh):
    dma = pltpu.SemaphoreType.DMA

    def step(x, w_gate, w_up, w_down):
        hbm = pl.BlockSpec(memory_space=pl.ANY)
        return pl.pallas_call(
            kernel,
            out_shape=pltpu.VMEM((R, D), BF),
            in_specs=[hbm] * 4,
            out_specs=pl.BlockSpec(memory_space=pltpu.VMEM),
            scratch_shapes=[
                pltpu.VMEM((4 * R, D), BF),
                pltpu.VMEM((4 * R, F), BF),
                pltpu.VMEM((2, D, 1024), BF),
                pltpu.VMEM((2 * R, 2 * F), F32),
                pltpu.VMEM((R, D), BF),
                pltpu.VMEM((R, D), BF),
                dma((2, 8)), dma,
                dma((2,)), dma((2,)),
                dma((NP,)), dma((NP,)),
                dma((NP,)), dma((NP,)),
                dma((NU,)), dma((NU,)),
                dma((NU,)), dma((NU,)),
                dma((ND // 2,)), dma((ND // 2,)),
            ],
            compiler_params=pltpu.CompilerParams(
                collective_id=0, has_side_effects=True, vmem_limit_bytes=64500000),
            name="mlp",
        )(x, w_gate, w_up, w_down)

    return jax.shard_map(
        step,
        mesh=mesh,
        in_specs=(P(("dp", "tp"), None), P(None, "tp"), P(None, "tp"), P("tp", None)),
        out_specs=P(("dp", "tp"), None),
        check_vma=False,
    )
```

```python
import jax
import jax.numpy as jnp
from jax import lax
from jax.experimental import pallas as pl
from jax.experimental.pallas import tpu as pltpu
from jax.sharding import PartitionSpec as P

D = 6144
F = 4096
R = 192
NB = 512
ND = D // NB
BF = jnp.bfloat16
F32 = jnp.float32
MESH = pl.DeviceIdType.MESH
PART = 1536
NP = D // PART

T_P = 5
T_FAR = T_P + 2 * NP
T_OWN = T_FAR + ND // 2 + 1
T_NEAR = T_OWN + 3
T_END = T_NEAR + ND // 2 - 1
RELAY = (3, T_P + 1, T_P + 3, T_P + 5)
NU = ND // 2 + 1


def kernel(x_hbm, wg, wu, wd, out, X, H, W, S, T, rD, rR,
           wsem, lsem, ps, pr, xs, xr, ys, yr, ds_, dr, rs, rr, qs, qr):
    me = lax.axis_index("tp")
    partner = me + 1 - 2 * lax.rem(me, 2)
    remote = lax.rem(me + 2, 4)

    def rcopy(src, dst, s, r, dev):
        return pltpu.make_async_remote_copy(
            src_ref=src, dst_ref=dst, send_sem=s, recv_sem=r,
            device_id={"tp": dev}, device_id_type=MESH)

    def load_own():
        return pltpu.make_async_copy(x_hbm, X.at[pl.ds(0, R), :], lsem)

    def to_partner(c):
        rows = R // 2
        return rcopy(x_hbm.at[pl.ds(c * rows, rows), :], X.at[pl.ds(R + c * rows, rows), :],
                     ps.at[c], pr.at[c], partner)

    def to_remote(k):
        c = pl.ds(k * PART, PART)
        return rcopy(x_hbm.at[:, c], X.at[pl.ds(2 * R, R), c], xs.at[k], xr.at[k], remote)

    def relay(k):
        c = pl.ds(k * PART, PART)
        return rcopy(X.at[pl.ds(2 * R, R), c], X.at[pl.ds(3 * R, R), c], ys.at[k], yr.at[k], partner)

    def block(i):
        return pl.ds(pl.multiple_of(i * 512, 512), 512)

    def own_copies(i, slot, halves=(0, 1), rows=pl.ds(0, D)):
        return [pltpu.make_async_copy(
            w.at[rows, pl.ds(pl.multiple_of(i * 512 + b * 256, 256), 256)],
            W.at[slot, rows, pl.ds(b * 512 + q * 256, 256)], wsem.at[slot, 2 * b + q])
            for b in halves for q, w in ((0, wg), (1, wu))]

    def part_copies(p, slot):
        rows = pl.ds(pl.multiple_of(p // 2 * PART, PART), PART)
        return [pltpu.make_async_copy(
            w.at[rows, block(p % 2 * 4 + e)],
            W.at[slot, pl.ds(e * PART, PART), pl.ds(q * 512, 512)], wsem.at[slot, 2 * e + q])
            for e in range(4) for q, w in ((0, wg), (1, wu))]

    def down_copy(pair, slot):
        c = pl.ds(pl.multiple_of(pair * 1024, 1024), 1024)
        return pltpu.make_async_copy(wd.at[:, c], W.at[slot, pl.ds(0, F), :], wsem.at[slot, 7])

    def own_block(t):
        return t - (T_OWN - T_P) * (t // T_OWN)

    def at(start, size):
        return pl.ds(start if isinstance(start, int) else pl.multiple_of(start, size), size)

    def cols(n):
        return at(n * NB, NB)

    def wide(n):
        return at(n * 1024, 1024)

    def dot(a, w):
        return jnp.dot(a, w, preferred_element_type=F32)

    def own(rows, m, slot, i, halves=(0, 1)):
        for b in halves:
            r = dot(X[pl.ds(rows, m), :], W[slot, :, pl.ds(b * 512, 512)])
            c = pl.ds(pl.multiple_of(i * 512 + b * 256, 256), 256)
            H[pl.ds(rows, m), c] = (jax.nn.silu(r[:, :256]) * r[:, 256:]).astype(BF)

    def part(slot, p, e, q):
        x = X[pl.ds(2 * R, 2 * R), pl.ds(pl.multiple_of(p // 2 * PART, PART), PART)]
        c = block((p % 2 * 4 + e) * 2 + q)
        return c, dot(x, W[slot, pl.ds(e * PART, PART), pl.ds(q * 512, 512)]) + S[:, c]

    KH = D // 2

    def quarter(b, k):
        rows = pl.ds(k * KH, KH)
        return [pltpu.make_async_copy(
            w.at[rows, pl.ds(b * 256, 256)],
            W.at[0, rows, pl.ds(b * 512 + q * 256, 256)], wsem.at[0, 4 * k + 2 * b + q])
            for q, w in ((0, wg), (1, wu))]

    def start_quarter(b, k):
        for c in quarter(b, k):
            c.start()

    def quarter_dot(b, k):
        for c in quarter(b, k):
            c.wait()
        rows = pl.ds(k * KH, KH)
        return dot(X[pl.ds(0, R), rows], W[0, rows, pl.ds(b * 512, 512)])

    load_own().start()
    start_quarter(0, 0)

    barrier = pltpu.get_barrier_semaphore()
    for dev in (partner, remote):
        pl.semaphore_signal(barrier, inc=1, device_id={"tp": dev}, device_id_type=MESH)

    def clear(k, carry):
        S[pl.ds(pl.multiple_of(k * 8, 8), 8), :] = jnp.zeros((8, 2 * F), F32)
        return carry

    lax.fori_loop(0, R // 8, clear, 0)
    start_quarter(0, 1)
    lax.fori_loop(R // 8, 2 * R // 8, clear, 0)
    start_quarter(1, 0)
    start_quarter(1, 1)
    pl.semaphore_wait(barrier, 2)
    for c in range(2):
        to_partner(c).start()
    for k in range(NP):
        to_remote(k).start()
    for c in own_copies(1, 1):
        c.start()
    load_own().wait()
    for b in range(2):
        T[...] = quarter_dot(b, 0)
        r = quarter_dot(b, 1) + T[...]
        H[pl.ds(0, R), pl.ds(b * 256, 256)] = (jax.nn.silu(r[:, :256]) * r[:, 256:]).astype(BF)
    for c in range(2):
        to_partner(c).wait_recv()
    own(R, R, 0, 0)

    def far_copy(u, rows, dst, s, r, dev, go):
        if isinstance(u, int):
            c = cols(u) if u < 2 else wide(u - 1)
            go(rcopy(X.at[rows, c], dst.at[:, c], s.at[u], r.at[u], dev))
            return

        @pl.when(u < 2)
        def _():
            c = cols(u)
            go(rcopy(X.at[rows, c], dst.at[:, c], s.at[u], r.at[u], dev))

        @pl.when(u >= 2)
        def _():
            c = wide(u - 1)
            go(rcopy(X.at[rows, c], dst.at[:, c], s.at[u], r.at[u], dev))

    def send_d(u, go):
        far_copy(u, pl.ds(2 * R, R), rD, ds_, dr, partner, go)

    def send_r(u, go):
        far_copy(u, pl.ds(3 * R, R), rR, rs, rr, remote, go)

    start = lambda c: c.start()
    wait_send = lambda c: c.wait_send()
    wait_recv = lambda c: c.wait_recv()

    def landing(n):
        return pl.ds(2 * R + n % 2 * R, R)

    def send_p(n):
        return rcopy(X.at[pl.ds(0, R), wide(n)], H.at[landing(n), wide(n // 2)], qs.at[n], qr.at[n], partner)

    def pair_sum(c, h):
        X[pl.ds(3 * R, R), c] = (S[pl.ds(R, R), h] + rD[:, c].astype(F32)).astype(BF)

    def down(rows, slot, w, keep_rows, keep, send_rows, c):
        r = dot(H[pl.ds(rows, 2 * R), :], W[slot, pl.ds(0, F), w])
        S[keep_rows, keep] = r[:R]
        X[send_rows, c] = r[R:].astype(BF)

    def step(t, carry):
        late = t // (T_FAR + 1) - t // (2 * T_FAR + 2)
        slot = lax.rem(t + late, 2)
        other = 1 - slot

        @pl.when(t < T_FAR)
        def _():
            @pl.when(t < T_P - 1)
            def _():
                for c in own_copies(t + 1, other):
                    c.start()

            @pl.when((t >= T_P - 1) & (t < T_FAR - 1))
            def _():
                for c in part_copies(t + 1 - T_P, other):
                    c.start()

            @pl.when(t == T_FAR - 1)
            def _():
                down_copy(0, other).start()

            @pl.when((t == RELAY[0]) | (t == RELAY[1]) | (t == RELAY[2]) | (t == RELAY[3]))
            def _():
                for k in range(NP):
                    @pl.when(t == RELAY[k])
                    def _(k=k):
                        to_remote(k).wait_recv()
                        relay(k).start()

            @pl.when(t >= T_P)
            def _():
                p = t - T_P

                @pl.when(lax.rem(p, 2) == 0)
                def _():
                    for k in range(NP):
                        @pl.when(p == 2 * k)
                        def _(k=k):
                            relay(k).wait_recv()

                for c in part_copies(p, slot):
                    c.wait()

                @pl.when(p < 2 * NP - 2)
                def _():
                    for e in range(4):
                        for q in range(2):
                            c, r = part(slot, p, e, q)
                            S[:, c] = r

                @pl.when(p >= 2 * NP - 2)
                def _():
                    for e in range(4):
                        c, r = part(slot, p, e, 0)
                        S[:, c] = jax.nn.silu(r)
                        up = part(slot, p, e, 1)[1]
                        H[pl.ds(2 * R, 2 * R), block(lax.rem(p, 2) * 4 + e)] = (S[:, c] * up).astype(BF)

        @pl.when((t >= T_FAR) & (t < T_NEAR))
        def _():
            u = t - T_FAR

            @pl.when(u == 0)
            def _():
                down_copy(1, other).start()
                for c in range(2):
                    to_partner(c).wait_send()
                for k in range(NP):
                    to_remote(k).wait_send()
                    relay(k).wait_send()

            @pl.when((u > 1) & (u < NU - 1))
            def _():
                down_copy(u, other).start()

            @pl.when(u == NU - 2)
            def _():
                for c in own_copies(T_P, slot, rows=pl.ds(F, D - F)):
                    c.start()

            @pl.when(u == NU - 1)
            def _():
                for c in own_copies(T_P, other, rows=pl.ds(0, F)):
                    c.start()

            @pl.when((u >= NU) & (u < NU + 2))
            def _():
                for c in own_copies(T_P + u - NU + 1, other):
                    c.start()

            @pl.when(u == NU + 2)
            def _():
                down_copy(0, other).start()

            @pl.when((u > 0) & (u <= NU))
            def _():
                send_d(u - 1, start)

            @pl.when((u > 1) & (u <= NU + 1))
            def _():
                send_r(u - 2, start)

            @pl.when(u < 2)
            def _():
                @pl.when(u == 0)
                def _():
                    down_copy(0, T_FAR % 2).wait()

                down(2 * R, T_FAR % 2, cols(u), pl.ds(R, R), cols(u), pl.ds(2 * R, R), cols(u))

        @pl.when((t < T_P) | ((t >= T_OWN) & (t < T_NEAR)))
        def _():
            i = own_block(t)
            for c in own_copies(i, slot):
                c.wait()
            own(0, 2 * R, slot, i)

        @pl.when(((t >= T_FAR + 2) & (t < T_OWN)) | (t >= T_NEAR))
        def _():
            near = t // T_NEAR
            m = t - T_FAR - 1 - (T_NEAR - T_FAR - 1) * near

            @pl.when(t >= T_NEAR)
            def _():
                down_copy(m + 1, other).start()

            @pl.when((t >= T_NEAR) & (m > 0))
            def _():
                send_p(m - 1).start()

            down_copy(m, slot).wait()
            far = 1 - near
            k = 2 * (lax.rem(m, 2) * far + m * near)
            for b in range(2):
                down(pl.multiple_of(2 * R * far, 128), slot, pl.ds(b * NB, NB),
                     pl.ds(pl.multiple_of(R * far, 64), R), cols(k + b),
                     pl.ds(pl.multiple_of(2 * R * far, 128), R), cols(2 * m + b))

        @pl.when((t > T_FAR) & (t <= T_OWN))
        def _():
            u = t - T_FAR - 1
            send_d(u, wait_recv)

            @pl.when(u < 2)
            def _():
                pair_sum(cols(u), cols(u))

            @pl.when(u >= 2)
            def _():
                pair_sum(wide(u - 1), wide(lax.rem(u - 1, 2)))

        return carry

    lax.fori_loop(1, T_END, step, 0)

    last = ND // 2 - 1

    def arrived(n):
        send_p(n).wait_recv()
        if n == 0:
            send_r(0, wait_recv)
        send_r(n + 1, wait_recv)

    def finish(n):
        out[:, wide(n)] = (S[pl.ds(0, R), wide(n)] + H[landing(n), wide(n // 2)].astype(F32)
                           + rR[:, wide(n)].astype(F32)).astype(BF)

    def last_dot(rows, b):
        return dot(H[pl.ds(rows, R), :], W[(T_END + 1) % 2, pl.ds(0, F), pl.ds(b * NB, NB)])

    def drain(u, carry):
        send_d(u, wait_send)
        send_r(u, wait_send)
        return carry

    send_p(last - 1).start()
    down_copy(last, (T_END + 1) % 2).wait()
    for b in range(2):
        X[pl.ds(0, R), cols(2 * last + b)] = last_dot(R, b).astype(BF)
    send_p(last).start()
    for b in range(2):
        S[pl.ds(0, R), cols(2 * last + b)] = last_dot(0, b)
    for n in range(last):
        arrived(n)
        finish(n)
    lax.fori_loop(0, NU - 1, drain, 0)
    arrived(last)
    finish(last)
    drain(NU - 1, 0)
    for n in range(last + 1):
        send_p(n).wait_send()


def solution(mesh):
    dma = pltpu.SemaphoreType.DMA

    def step(x, w_gate, w_up, w_down):
        hbm = pl.BlockSpec(memory_space=pl.ANY)
        return pl.pallas_call(
            kernel,
            out_shape=pltpu.VMEM((R, D), BF),
            in_specs=[hbm] * 4,
            out_specs=pl.BlockSpec(memory_space=pltpu.VMEM),
            scratch_shapes=[
                pltpu.VMEM((4 * R, D), BF),
                pltpu.VMEM((4 * R, F), BF),
                pltpu.VMEM((2, D, 1024), BF),
                pltpu.VMEM((2 * R, 2 * F), F32),
                pltpu.VMEM((R, NB), F32),
                pltpu.VMEM((R, D), BF),
                pltpu.VMEM((R, D), BF),
                dma((2, 8)), dma,
                dma((2,)), dma((2,)),
                dma((NP,)), dma((NP,)),
                dma((NP,)), dma((NP,)),
                dma((NU,)), dma((NU,)),
                dma((NU,)), dma((NU,)),
                dma((ND // 2,)), dma((ND // 2,)),
            ],
            compiler_params=pltpu.CompilerParams(
                collective_id=0, has_side_effects=True, vmem_limit_bytes=64500000),
            name="mlp",
        )(x, w_gate, w_up, w_down)

    return jax.shard_map(
        step,
        mesh=mesh,
        in_specs=(P(("dp", "tp"), None), P(None, "tp"), P(None, "tp"), P("tp", None)),
        out_specs=P(("dp", "tp"), None),
        check_vma=False,
    )
```

```python
import jax
import jax.numpy as jnp
from jax import lax
from jax.experimental import pallas as pl
from jax.experimental.pallas import tpu as pltpu
from jax.sharding import PartitionSpec as P

D = 6144
F = 4096
R = 192
NB = 512
ND = D // NB
BF = jnp.bfloat16
F32 = jnp.float32
MESH = pl.DeviceIdType.MESH
PART = 1536
NP = D // PART

NT = ND // 3
NU = 3 + NT - 1
T_P = 5
T_FAR = T_P + 2 * NP
T_OWN = T_FAR + NU
T_NEAR = T_OWN + 3
T_END = T_NEAR + NT - 1
RELAY = (3, T_P + 1, T_P + 3, T_P + 5)


def kernel(x_hbm, wg, wu, wd, out, X, H, W, S, T, rD, rR,
           wsem, lsem, ps, pr, xs, xr, ys, yr, ds_, dr, rs, rr, qs, qr):
    me = lax.axis_index("tp")
    partner = me + 1 - 2 * lax.rem(me, 2)
    remote = lax.rem(me + 2, 4)

    def rcopy(src, dst, s, r, dev):
        return pltpu.make_async_remote_copy(
            src_ref=src, dst_ref=dst, send_sem=s, recv_sem=r,
            device_id={"tp": dev}, device_id_type=MESH)

    def load_own():
        return pltpu.make_async_copy(x_hbm, X.at[pl.ds(0, R), :], lsem)

    def to_partner(c):
        rows = R // 2
        return rcopy(x_hbm.at[pl.ds(c * rows, rows), :], X.at[pl.ds(R + c * rows, rows), :],
                     ps.at[c], pr.at[c], partner)

    def to_remote(k):
        c = pl.ds(k * PART, PART)
        return rcopy(x_hbm.at[:, c], X.at[pl.ds(2 * R, R), c], xs.at[k], xr.at[k], remote)

    def relay(k):
        c = pl.ds(k * PART, PART)
        return rcopy(X.at[pl.ds(2 * R, R), c], X.at[pl.ds(3 * R, R), c], ys.at[k], yr.at[k], partner)

    def block(i):
        return pl.ds(pl.multiple_of(i * 512, 512), 512)

    def own_copies(i, slot):
        return [pltpu.make_async_copy(
            w.at[:, pl.ds(pl.multiple_of(i * 512 + b * 256, 256), 256)],
            W.at[slot, :, pl.ds(b * 512 + q * 256, 256)], wsem.at[slot, 2 * b + q])
            for b in range(2) for q, w in ((0, wg), (1, wu))]

    def part_copies(p, slot):
        rows = pl.ds(pl.multiple_of(p // 2 * PART, PART), PART)
        return [pltpu.make_async_copy(
            w.at[rows, block(p % 2 * 4 + e)],
            W.at[slot, pl.ds(e * PART, PART), pl.ds(q * 512, 512)], wsem.at[slot, 2 * e + q])
            for e in range(4) for q, w in ((0, wg), (1, wu))]

    def down_copies(g, slot):
        two = pl.ds(pl.multiple_of(g * 3 * NB, NB), 2 * NB)
        third = pl.ds(pl.multiple_of(g * 3 * NB + 2 * NB, NB), NB)
        return [pltpu.make_async_copy(wd.at[:, two], W.at[slot, pl.ds(0, F), :], wsem.at[slot, 5])] + [
            pltpu.make_async_copy(
                wd.at[pl.ds(k * F // 2, F // 2), third],
                W.at[slot, pl.ds(F, F // 2), pl.ds(k * NB, NB)], wsem.at[slot, 6 + k])
            for k in range(2)]

    def start_down(g, slot):
        for c in down_copies(g, slot):
            c.start()

    def wait_down(g, slot):
        for c in down_copies(g, slot):
            c.wait()

    def own_block(t):
        return t - (T_OWN - T_P) * (t // T_OWN)

    def at(start, size):
        return pl.ds(start if isinstance(start, int) else pl.multiple_of(start, size), size)

    def cols(n):
        return at(n * NB, NB)

    def tri(n):
        return at(n * 3 * NB, 3 * NB)

    def dot(a, w):
        return jnp.dot(a, w, preferred_element_type=F32)

    def own(rows, m, slot, i):
        for b in range(2):
            r = dot(X[pl.ds(rows, m), :], W[slot, :, pl.ds(b * 512, 512)])
            c = pl.ds(pl.multiple_of(i * 512 + b * 256, 256), 256)
            H[pl.ds(rows, m), c] = (jax.nn.silu(r[:, :256]) * r[:, 256:]).astype(BF)

    def part(slot, p, e, q):
        x = X[pl.ds(2 * R, 2 * R), pl.ds(pl.multiple_of(p // 2 * PART, PART), PART)]
        c = block((p % 2 * 4 + e) * 2 + q)
        return c, dot(x, W[slot, pl.ds(e * PART, PART), pl.ds(q * 512, 512)]) + S[:, c]

    KH = D // 2

    def quarter(b, k):
        rows = pl.ds(k * KH, KH)
        return [pltpu.make_async_copy(
            w.at[rows, pl.ds(b * 256, 256)],
            W.at[0, rows, pl.ds(b * 512 + q * 256, 256)], wsem.at[0, 4 * k + 2 * b + q])
            for q, w in ((0, wg), (1, wu))]

    def start_quarter(b, k):
        for c in quarter(b, k):
            c.start()

    def quarter_dot(b, k):
        for c in quarter(b, k):
            c.wait()
        rows = pl.ds(k * KH, KH)
        return dot(X[pl.ds(0, R), rows], W[0, rows, pl.ds(b * 512, 512)])

    load_own().start()
    start_quarter(0, 0)

    barrier = pltpu.get_barrier_semaphore()
    for dev in (partner, remote):
        pl.semaphore_signal(barrier, inc=1, device_id={"tp": dev}, device_id_type=MESH)

    def clear(k, carry):
        S[pl.ds(pl.multiple_of(k * 8, 8), 8), :] = jnp.zeros((8, 2 * F), F32)
        return carry

    lax.fori_loop(0, R // 8, clear, 0)
    start_quarter(0, 1)
    lax.fori_loop(R // 8, 2 * R // 8, clear, 0)
    start_quarter(1, 0)
    start_quarter(1, 1)
    pl.semaphore_wait(barrier, 2)
    for c in range(2):
        to_partner(c).start()
    for k in range(NP):
        to_remote(k).start()
    for c in own_copies(1, 1):
        c.start()
    load_own().wait()
    for b in range(2):
        T[...] = quarter_dot(b, 0)
        r = quarter_dot(b, 1) + T[...]
        H[pl.ds(0, R), pl.ds(b * 256, 256)] = (jax.nn.silu(r[:, :256]) * r[:, 256:]).astype(BF)
    for c in range(2):
        to_partner(c).wait_recv()
    own(R, R, 0, 0)

    def far_copy(u, rows, dst, s, r, dev, go):
        if isinstance(u, int):
            c = cols(u) if u < 3 else tri(u - 2)
            go(rcopy(X.at[rows, c], dst.at[:, c], s.at[u], r.at[u], dev))
            return

        @pl.when(u < 3)
        def _():
            c = cols(u)
            go(rcopy(X.at[rows, c], dst.at[:, c], s.at[u], r.at[u], dev))

        @pl.when(u >= 3)
        def _():
            c = tri(u - 2)
            go(rcopy(X.at[rows, c], dst.at[:, c], s.at[u], r.at[u], dev))

    def send_d(u, go):
        far_copy(u, pl.ds(2 * R, R), rD, ds_, dr, partner, go)

    def send_r(u, go):
        far_copy(u, pl.ds(3 * R, R), rR, rs, rr, remote, go)

    start = lambda c: c.start()
    wait_send = lambda c: c.wait_send()
    wait_recv = lambda c: c.wait_recv()

    def landing(n):
        return pl.ds(2 * R + n % 2 * R, R)

    def send_p(n):
        return rcopy(X.at[pl.ds(0, R), tri(n)], H.at[landing(n), tri(n // 2)], qs.at[n], qr.at[n], partner)

    def pair_sum(c, h):
        X[pl.ds(3 * R, R), c] = (S[pl.ds(R, R), h] + rD[:, c].astype(F32)).astype(BF)

    def down_dot(rows, m, slot, b):
        if isinstance(b, int) and b == 2:
            r = [dot(H[pl.ds(rows, m), pl.ds(k * F // 2, F // 2)],
                     W[slot, pl.ds(F, F // 2), pl.ds(k * NB, NB)]) for k in range(2)]
            return r[0] + r[1]
        return dot(H[pl.ds(rows, m), :], W[slot, pl.ds(0, F), cols(b)])

    def down(rows, slot, b, keep_rows, keep, send_rows, c):
        r = down_dot(rows, 2 * R, slot, b)
        S[keep_rows, keep] = r[:R]
        X[send_rows, c] = r[R:].astype(BF)

    def step(t, carry):
        slot = lax.rem(t, 2)
        other = 1 - slot

        @pl.when(t < T_FAR)
        def _():
            @pl.when(t < T_P - 1)
            def _():
                for c in own_copies(t + 1, other):
                    c.start()

            @pl.when((t >= T_P - 1) & (t < T_FAR - 1))
            def _():
                for c in part_copies(t + 1 - T_P, other):
                    c.start()

            @pl.when(t == T_FAR - 1)
            def _():
                start_down(0, other)

            @pl.when((t == RELAY[0]) | (t == RELAY[1]) | (t == RELAY[2]) | (t == RELAY[3]))
            def _():
                for k in range(NP):
                    @pl.when(t == RELAY[k])
                    def _(k=k):
                        to_remote(k).wait_recv()
                        relay(k).start()

            @pl.when(t >= T_P)
            def _():
                p = t - T_P

                @pl.when(lax.rem(p, 2) == 0)
                def _():
                    for k in range(NP):
                        @pl.when(p == 2 * k)
                        def _(k=k):
                            relay(k).wait_recv()

                for c in part_copies(p, slot):
                    c.wait()

                @pl.when(p < 2 * NP - 2)
                def _():
                    for e in range(4):
                        for q in range(2):
                            c, r = part(slot, p, e, q)
                            S[:, c] = r

                @pl.when(p >= 2 * NP - 2)
                def _():
                    for e in range(4):
                        c, r = part(slot, p, e, 0)
                        S[:, c] = jax.nn.silu(r)
                        up = part(slot, p, e, 1)[1]
                        H[pl.ds(2 * R, 2 * R), block(lax.rem(p, 2) * 4 + e)] = (S[:, c] * up).astype(BF)

        @pl.when((t >= T_FAR) & (t < T_NEAR))
        def _():
            u = t - T_FAR

            @pl.when(u == 0)
            def _():
                start_down(1, other)
                for c in range(2):
                    to_partner(c).wait_send()
                for k in range(NP):
                    to_remote(k).wait_send()
                    relay(k).wait_send()

            @pl.when((u > 2) & (u < NU - 1))
            def _():
                start_down(u - 1, other)

            @pl.when((u >= NU - 1) & (u < NU + 2))
            def _():
                for c in own_copies(T_P + u - NU + 1, other):
                    c.start()

            @pl.when(u == NU + 2)
            def _():
                start_down(0, other)

            @pl.when((u > 0) & (u <= NU))
            def _():
                send_d(u - 1, start)

            @pl.when((u > 1) & (u <= NU + 1))
            def _():
                send_r(u - 2, start)

            def single(b):
                down(2 * R, T_FAR % 2, b, pl.ds(R, R), cols(b), pl.ds(2 * R, R), cols(b))

            @pl.when(u < 2)
            def _():
                @pl.when(u == 0)
                def _():
                    wait_down(0, T_FAR % 2)

                single(u)

            @pl.when(u == 2)
            def _():
                single(2)

        @pl.when((t < T_P) | ((t >= T_OWN) & (t < T_NEAR)))
        def _():
            i = own_block(t)
            for c in own_copies(i, slot):
                c.wait()
            own(0, 2 * R, slot, i)

        @pl.when(((t >= T_FAR + 3) & (t < T_OWN)) | (t >= T_NEAR))
        def _():
            near = t // T_NEAR
            far = 1 - near
            g = t - T_FAR - 2 - (T_NEAR - T_FAR - 2) * near

            @pl.when(t >= T_NEAR)
            def _():
                start_down(g + 1, other)

            @pl.when((t >= T_NEAR) & (g > 0))
            def _():
                send_p(g - 1).start()

            wait_down(g, slot)
            k = 3 * (lax.rem(g, 2) * far + g * near)
            for b in range(3):
                down(pl.multiple_of(2 * R * far, 128), slot, b,
                     pl.ds(pl.multiple_of(R * far, 64), R), cols(k + b),
                     pl.ds(pl.multiple_of(2 * R * far, 128), R), cols(3 * g + b))

        @pl.when((t > T_FAR) & (t <= T_OWN))
        def _():
            u = t - T_FAR - 1
            send_d(u, wait_recv)

            @pl.when(u < 3)
            def _():
                pair_sum(cols(u), cols(u))

            @pl.when(u >= 3)
            def _():
                pair_sum(tri(u - 2), tri(lax.rem(u, 2)))

        return carry

    lax.fori_loop(1, T_END, step, 0)

    last = NT - 1

    def arrived(n):
        send_p(n).wait_recv()
        for u in (0, 1, 2) if n == 0 else (n + 2,):
            send_r(u, wait_recv)

    def finish(n):
        out[:, tri(n)] = (S[pl.ds(0, R), tri(n)] + H[landing(n), tri(n // 2)].astype(F32)
                          + rR[:, tri(n)].astype(F32)).astype(BF)

    def drain(u, carry):
        send_d(u, wait_send)
        send_r(u, wait_send)
        return carry

    send_p(last - 1).start()
    wait_down(last, T_END % 2)
    for b in range(3):
        X[pl.ds(0, R), cols(3 * last + b)] = down_dot(R, R, T_END % 2, b).astype(BF)
    send_p(last).start()
    for b in range(3):
        S[pl.ds(0, R), cols(3 * last + b)] = down_dot(0, R, T_END % 2, b)
    for n in range(last):
        arrived(n)
        finish(n)
    lax.fori_loop(0, NU - 1, drain, 0)
    arrived(last)
    finish(last)
    drain(NU - 1, 0)
    for n in range(last + 1):
        send_p(n).wait_send()


def solution(mesh):
    dma = pltpu.SemaphoreType.DMA

    def step(x, w_gate, w_up, w_down):
        hbm = pl.BlockSpec(memory_space=pl.ANY)
        return pl.pallas_call(
            kernel,
            out_shape=pltpu.VMEM((R, D), BF),
            in_specs=[hbm] * 4,
            out_specs=pl.BlockSpec(memory_space=pltpu.VMEM),
            scratch_shapes=[
                pltpu.VMEM((4 * R, D), BF),
                pltpu.VMEM((4 * R, F), BF),
                pltpu.VMEM((2, D, 1024), BF),
                pltpu.VMEM((2 * R, 2 * F), F32),
                pltpu.VMEM((R, NB), F32),
                pltpu.VMEM((R, D), BF),
                pltpu.VMEM((R, D), BF),
                dma((2, 8)), dma,
                dma((2,)), dma((2,)),
                dma((NP,)), dma((NP,)),
                dma((NP,)), dma((NP,)),
                dma((NU,)), dma((NU,)),
                dma((NU,)), dma((NU,)),
                dma((NT,)), dma((NT,)),
            ],
            compiler_params=pltpu.CompilerParams(
                collective_id=0, has_side_effects=True, vmem_limit_bytes=64500000),
            name="mlp",
        )(x, w_gate, w_up, w_down)

    return jax.shard_map(
        step,
        mesh=mesh,
        in_specs=(P(("dp", "tp"), None), P(None, "tp"), P(None, "tp"), P("tp", None)),
        out_specs=P(("dp", "tp"), None),
        check_vma=False,
    )
```

```python
import jax
import jax.numpy as jnp
from jax import lax
from jax.experimental import pallas as pl
from jax.experimental.pallas import tpu as pltpu
from jax.sharding import PartitionSpec as P

D = 6144
F = 4096
R = 192
NB = 512
ND = D // NB
BF = jnp.bfloat16
F32 = jnp.float32
MESH = pl.DeviceIdType.MESH
PART = 1536
NP = D // PART

NT = ND // 3
NU = 3 + NT - 1
T_P = 5
T_FAR = T_P + 2 * NP
T_OWN = T_FAR + NU
T_NEAR = T_OWN + 3
T_END = T_NEAR + NT - 1
RELAY = (3, T_P + 1, T_P + 3, T_P + 5)


def kernel(x_hbm, wg, wu, wd, out, X, H, W, S, T, rD, rR,
           wsem, lsem, ps, pr, xs, xr, ys, yr, ds_, dr, rs, rr, qs, qr):
    me = lax.axis_index("tp")
    partner = me + 1 - 2 * lax.rem(me, 2)
    remote = lax.rem(me + 2, 4)

    def rcopy(src, dst, s, r, dev):
        return pltpu.make_async_remote_copy(
            src_ref=src, dst_ref=dst, send_sem=s, recv_sem=r,
            device_id={"tp": dev}, device_id_type=MESH)

    def load_own():
        return pltpu.make_async_copy(x_hbm, X.at[pl.ds(0, R), :], lsem)

    def to_partner(c):
        rows = R // 2
        return rcopy(x_hbm.at[pl.ds(c * rows, rows), :], X.at[pl.ds(R + c * rows, rows), :],
                     ps.at[c], pr.at[c], partner)

    def to_remote(k):
        c = pl.ds(k * PART, PART)
        return rcopy(x_hbm.at[:, c], X.at[pl.ds(2 * R, R), c], xs.at[k], xr.at[k], remote)

    def relay(k):
        c = pl.ds(k * PART, PART)
        return rcopy(X.at[pl.ds(2 * R, R), c], X.at[pl.ds(3 * R, R), c], ys.at[k], yr.at[k], partner)

    def block(i):
        return pl.ds(pl.multiple_of(i * 512, 512), 512)

    def own_copies(i, slot):
        return [pltpu.make_async_copy(
            w.at[:, pl.ds(pl.multiple_of(i * 512 + b * 256, 256), 256)],
            W.at[slot, :, pl.ds(b * 512 + q * 256, 256)], wsem.at[slot, 2 * b + q])
            for b in range(2) for q, w in ((0, wg), (1, wu))]

    def part_copies(p, slot):
        rows = pl.ds(pl.multiple_of(p // 2 * PART, PART), PART)
        return [pltpu.make_async_copy(
            w.at[rows, block(p % 2 * 4 + e)],
            W.at[slot, pl.ds(e * PART, PART), pl.ds(q * 512, 512)], wsem.at[slot, 2 * e + q])
            for e in range(4) for q, w in ((0, wg), (1, wu))]

    def down_copies(g, slot):
        two = pl.ds(pl.multiple_of(g * 3 * NB, NB), 2 * NB)
        third = pl.ds(pl.multiple_of(g * 3 * NB + 2 * NB, NB), NB)
        return [pltpu.make_async_copy(wd.at[:, two], W.at[slot, pl.ds(0, F), :], wsem.at[slot, 5])] + [
            pltpu.make_async_copy(
                wd.at[pl.ds(k * F // 2, F // 2), third],
                W.at[slot, pl.ds(F, F // 2), pl.ds(k * NB, NB)], wsem.at[slot, 6 + k])
            for k in range(2)]

    def start_down(g, slot):
        for c in down_copies(g, slot):
            c.start()

    def wait_down(g, slot):
        for c in down_copies(g, slot):
            c.wait()

    def own_block(t):
        return t - (T_OWN - T_P) * (t // T_OWN)

    def at(start, size):
        return pl.ds(start if isinstance(start, int) else pl.multiple_of(start, size), size)

    def cols(n):
        return at(n * NB, NB)

    def tri(n):
        return at(n * 3 * NB, 3 * NB)

    def dot(a, w):
        return jnp.dot(a, w, preferred_element_type=F32)

    def own(rows, m, slot, i):
        for b in range(2):
            r = dot(X[pl.ds(rows, m), :], W[slot, :, pl.ds(b * 512, 512)])
            c = pl.ds(pl.multiple_of(i * 512 + b * 256, 256), 256)
            H[pl.ds(rows, m), c] = (jax.nn.silu(r[:, :256]) * r[:, 256:]).astype(BF)

    def part(slot, p, e, q):
        x = X[pl.ds(2 * R, 2 * R), pl.ds(pl.multiple_of(p // 2 * PART, PART), PART)]
        c = block((p % 2 * 4 + e) * 2 + q)
        return c, dot(x, W[slot, pl.ds(e * PART, PART), pl.ds(q * 512, 512)]) + S[:, c]

    KH = D // 2

    def quarter(b, k):
        rows = pl.ds(k * KH, KH)
        return [pltpu.make_async_copy(
            w.at[rows, pl.ds(b * 256, 256)],
            W.at[0, rows, pl.ds(b * 512 + q * 256, 256)], wsem.at[0, 4 * k + 2 * b + q])
            for q, w in ((0, wg), (1, wu))]

    def start_quarter(b, k):
        for c in quarter(b, k):
            c.start()

    def quarter_dot(b, k):
        for c in quarter(b, k):
            c.wait()
        rows = pl.ds(k * KH, KH)
        return dot(X[pl.ds(0, R), rows], W[0, rows, pl.ds(b * 512, 512)])

    load_own().start()
    start_quarter(0, 0)

    barrier = pltpu.get_barrier_semaphore()
    for dev in (partner, remote):
        pl.semaphore_signal(barrier, inc=1, device_id={"tp": dev}, device_id_type=MESH)

    def clear(k, carry):
        S[pl.ds(pl.multiple_of(k * 8, 8), 8), :] = jnp.zeros((8, 2 * F), F32)
        return carry

    lax.fori_loop(0, R // 8, clear, 0)
    start_quarter(0, 1)
    lax.fori_loop(R // 8, 2 * R // 8, clear, 0)
    start_quarter(1, 0)
    start_quarter(1, 1)
    pl.semaphore_wait(barrier, 2)
    for c in range(2):
        to_partner(c).start()
    for k in range(NP):
        to_remote(k).start()
    for c in own_copies(1, 1):
        c.start()
    load_own().wait()
    for b in range(2):
        T[...] = quarter_dot(b, 0)
        r = quarter_dot(b, 1) + T[...]
        H[pl.ds(0, R), pl.ds(b * 256, 256)] = (jax.nn.silu(r[:, :256]) * r[:, 256:]).astype(BF)
    for c in range(2):
        to_partner(c).wait_recv()
    own(R, R, 0, 0)

    def far_copy(u, rows, dst, s, r, dev, go):
        if isinstance(u, int):
            c = cols(u) if u < 3 else tri(u - 2)
            go(rcopy(X.at[rows, c], dst.at[:, c], s.at[u], r.at[u], dev))
            return

        @pl.when(u < 3)
        def _():
            c = cols(u)
            go(rcopy(X.at[rows, c], dst.at[:, c], s.at[u], r.at[u], dev))

        @pl.when(u >= 3)
        def _():
            c = tri(u - 2)
            go(rcopy(X.at[rows, c], dst.at[:, c], s.at[u], r.at[u], dev))

    def send_d(u, go):
        far_copy(u, pl.ds(2 * R, R), rD, ds_, dr, partner, go)

    def send_r(u, go):
        far_copy(u, pl.ds(3 * R, R), rR, rs, rr, remote, go)

    start = lambda c: c.start()
    wait_send = lambda c: c.wait_send()
    wait_recv = lambda c: c.wait_recv()

    def landing(n):
        return pl.ds(2 * R + n % 2 * R, R)

    def send_p(n):
        return rcopy(X.at[pl.ds(0, R), tri(n)], H.at[landing(n), tri(n // 2)], qs.at[n], qr.at[n], partner)

    def pair_sum(c, h):
        X[pl.ds(3 * R, R), c] = (S[pl.ds(R, R), h] + rD[:, c].astype(F32)).astype(BF)

    def down_dot(rows, m, slot, b):
        if isinstance(b, int) and b == 2:
            r = [dot(H[pl.ds(rows, m), pl.ds(k * F // 2, F // 2)],
                     W[slot, pl.ds(F, F // 2), pl.ds(k * NB, NB)]) for k in range(2)]
            return r[0] + r[1]
        return dot(H[pl.ds(rows, m), :], W[slot, pl.ds(0, F), cols(b)])

    def down(rows, slot, b, keep_rows, keep, send_rows, c):
        r = down_dot(rows, 2 * R, slot, b)
        S[keep_rows, keep] = r[:R]
        X[send_rows, c] = r[R:].astype(BF)

    def step(t, carry):
        slot = lax.rem(t, 2)
        other = 1 - slot

        @pl.when(t < T_FAR)
        def _():
            @pl.when(t < T_P - 1)
            def _():
                for c in own_copies(t + 1, other):
                    c.start()

            @pl.when((t >= T_P - 1) & (t < T_FAR - 1))
            def _():
                for c in part_copies(t + 1 - T_P, other):
                    c.start()

            @pl.when(t == T_FAR - 1)
            def _():
                start_down(0, other)

            @pl.when((t == RELAY[0]) | (t == RELAY[1]) | (t == RELAY[2]) | (t == RELAY[3]))
            def _():
                for k in range(NP):
                    @pl.when(t == RELAY[k])
                    def _(k=k):
                        to_remote(k).wait_recv()
                        relay(k).start()

            @pl.when(t >= T_P)
            def _():
                p = t - T_P

                @pl.when(lax.rem(p, 2) == 0)
                def _():
                    for k in range(NP):
                        @pl.when(p == 2 * k)
                        def _(k=k):
                            relay(k).wait_recv()

                for c in part_copies(p, slot):
                    c.wait()

                @pl.when(p < 2 * NP - 2)
                def _():
                    for e in range(4):
                        for q in range(2):
                            c, r = part(slot, p, e, q)
                            S[:, c] = r

                @pl.when(p >= 2 * NP - 2)
                def _():
                    for e in range(4):
                        gate = jax.nn.silu(part(slot, p, e, 0)[1])
                        up = part(slot, p, e, 1)[1]
                        H[pl.ds(2 * R, 2 * R), block(lax.rem(p, 2) * 4 + e)] = (gate * up).astype(BF)

        @pl.when((t >= T_FAR) & (t < T_NEAR))
        def _():
            u = t - T_FAR

            @pl.when(u == 0)
            def _():
                start_down(1, other)
                for c in range(2):
                    to_partner(c).wait_send()
                for k in range(NP):
                    to_remote(k).wait_send()
                    relay(k).wait_send()

            @pl.when((u > 2) & (u < NU - 1))
            def _():
                start_down(u - 1, other)

            @pl.when((u >= NU - 1) & (u < NU + 2))
            def _():
                for c in own_copies(T_P + u - NU + 1, other):
                    c.start()

            @pl.when(u == NU + 2)
            def _():
                start_down(0, other)

            @pl.when((u > 0) & (u <= NU))
            def _():
                send_d(u - 1, start)

            @pl.when((u > 1) & (u <= NU + 1))
            def _():
                send_r(u - 2, start)

            def single(b):
                down(2 * R, T_FAR % 2, b, pl.ds(R, R), cols(b), pl.ds(2 * R, R), cols(b))

            @pl.when(u < 2)
            def _():
                @pl.when(u == 0)
                def _():
                    wait_down(0, T_FAR % 2)

                single(u)

            @pl.when(u == 2)
            def _():
                single(2)

        @pl.when((t < T_P) | ((t >= T_OWN) & (t < T_NEAR)))
        def _():
            i = own_block(t)
            for c in own_copies(i, slot):
                c.wait()
            own(0, 2 * R, slot, i)

        @pl.when(((t >= T_FAR + 3) & (t < T_OWN)) | (t >= T_NEAR))
        def _():
            near = t // T_NEAR
            far = 1 - near
            g = t - T_FAR - 2 - (T_NEAR - T_FAR - 2) * near

            @pl.when(t >= T_NEAR)
            def _():
                start_down(g + 1, other)

            @pl.when((t >= T_NEAR) & (g > 0))
            def _():
                send_p(g - 1).start()

            wait_down(g, slot)
            k = 3 * (lax.rem(g, 2) * far + g * near)
            for b in range(3):
                down(pl.multiple_of(2 * R * far, 128), slot, b,
                     pl.ds(pl.multiple_of(R * far, 64), R), cols(k + b),
                     pl.ds(pl.multiple_of(2 * R * far, 128), R), cols(3 * g + b))

        @pl.when((t > T_FAR) & (t <= T_OWN))
        def _():
            u = t - T_FAR - 1
            send_d(u, wait_recv)

            @pl.when(u < 3)
            def _():
                pair_sum(cols(u), cols(u))

            @pl.when(u >= 3)
            def _():
                pair_sum(tri(u - 2), tri(lax.rem(u, 2)))

        return carry

    lax.fori_loop(1, T_END, step, 0)

    last = NT - 1

    def arrived(n):
        send_p(n).wait_recv()
        for u in (0, 1, 2) if n == 0 else (n + 2,):
            send_r(u, wait_recv)

    def finish(n):
        out[:, tri(n)] = (S[pl.ds(0, R), tri(n)] + H[landing(n), tri(n // 2)].astype(F32)
                          + rR[:, tri(n)].astype(F32)).astype(BF)

    def drain(u, carry):
        send_d(u, wait_send)
        send_r(u, wait_send)
        return carry

    send_p(last - 1).start()
    wait_down(last, T_END % 2)
    for b in range(3):
        X[pl.ds(0, R), cols(3 * last + b)] = down_dot(R, R, T_END % 2, b).astype(BF)
    send_p(last).start()
    for b in range(3):
        S[pl.ds(0, R), cols(3 * last + b)] = down_dot(0, R, T_END % 2, b)
    for n in range(last):
        arrived(n)
        finish(n)
    lax.fori_loop(0, NU - 1, drain, 0)
    arrived(last)
    finish(last)
    drain(NU - 1, 0)
    for n in range(last + 1):
        send_p(n).wait_send()


def solution(mesh):
    dma = pltpu.SemaphoreType.DMA

    def step(x, w_gate, w_up, w_down):
        hbm = pl.BlockSpec(memory_space=pl.ANY)
        return pl.pallas_call(
            kernel,
            out_shape=pltpu.VMEM((R, D), BF),
            in_specs=[hbm] * 4,
            out_specs=pl.BlockSpec(memory_space=pltpu.VMEM),
            scratch_shapes=[
                pltpu.VMEM((4 * R, D), BF),
                pltpu.VMEM((4 * R, F), BF),
                pltpu.VMEM((2, D, 1024), BF),
                pltpu.VMEM((2 * R, 2 * F), F32),
                pltpu.VMEM((R, NB), F32),
                pltpu.VMEM((R, D), BF),
                pltpu.VMEM((R, D), BF),
                dma((2, 8)), dma,
                dma((2,)), dma((2,)),
                dma((NP,)), dma((NP,)),
                dma((NP,)), dma((NP,)),
                dma((NU,)), dma((NU,)),
                dma((NU,)), dma((NU,)),
                dma((NT,)), dma((NT,)),
            ],
            compiler_params=pltpu.CompilerParams(
                collective_id=0, has_side_effects=True, vmem_limit_bytes=64500000),
            name="mlp",
        )(x, w_gate, w_up, w_down)

    return jax.shard_map(
        step,
        mesh=mesh,
        in_specs=(P(("dp", "tp"), None), P(None, "tp"), P(None, "tp"), P("tp", None)),
        out_specs=P(("dp", "tp"), None),
        check_vma=False,
    )
```
